256 devices in a mesh: gx: 16 (over y, x), gy: 2 (over core), gz: 8 (over z).
Axes of the slice: x: 4, y: 4, z: 8, core: 2. Of those that a mesh axis runs over, the one named last changes fastest.
Arguments:
- right_side: float32 [81, 64, 16, 1024], P(None, 'gx', 'gy', 'gz'), may hold values from -18 to 18
- cell_coef: float32 [64, 16, 256], P('gx', 'gy', 'gz'), may hold values from 0.5 to 2
- cell_matrix: float32 [81, 81], replicated, may hold values from -2 to 16, as said below
- face_coupling: float32 [3, 81, 81], replicated, may hold values from -0.18 to 0.18
- patch_inverse: bfloat16 [648, 648], replicated, may hold values from -0.01 to 0.1, as said below
Outputs:
- solution: float32 [81, 64, 16, 1024], P(None, 'gx', 'gy', 'gz')
- residual: float32 [81, 64, 16, 1024], P(None, 'gx', 'gy', 'gz')
The draws below stay inside these ranges and needn't reach their ends.
Inputs may be any that keep to these rules, and one draw needn't show every extreme that they name: `cell_matrix`: symmetric. `patch_inverse`: symmetric.
All inputs are finite; a program needn't handle non-finite values.
Results may differ from the reference program's by a relative error of at most 0.035.
Values may be sent and summed in bfloat16 or wider, within the bound.
A program may use at most 192 MiB of HBM per device.

```python
import math
import jax
import jax.numpy as jnp
from jax import lax

Q = 81
PATCH = 648
RHS = 4
NX = 64
NY = 16
NZ = 256


def symmetric_part(key, matrix_order):
    sampled = jnp.clip(jax.random.normal(key, (matrix_order, matrix_order), jnp.float32), -4.0, 4.0)
    return (sampled + sampled.T) * 0.7071


def draw_cell_matrix(key, part):
    key_diag = jax.random.fold_in(key, 11)
    key_rest = jax.random.fold_in(key, 12)
    diagonal = jax.random.uniform(key_diag, (Q,), jnp.float32, 10.8, 13.2)
    return jnp.diag(diagonal) + 0.35 * symmetric_part(key_rest, Q)


def draw_patch_inverse(key, part):
    key_diag = jax.random.fold_in(key, 21)
    key_rest = jax.random.fold_in(key, 22)
    diagonal = jax.random.uniform(key_diag, (PATCH,), jnp.float32, 0.9, 1.1)
    values = (jnp.diag(diagonal) + 0.012 * symmetric_part(key_rest, PATCH)) / 12.0
    return values.astype(jnp.bfloat16)


def shard_levels(stream_key, extent, split, low, largest):
    gain, own = 1.0, jax.random.fold_in(stream_key, 6)
    for position, parts in split:
        draws = jnp.exp(jax.random.uniform(jax.random.fold_in(own, position), (parts,), jnp.float32, low / len(split), largest / len(split)))
        gain = gain * jnp.repeat(draws, extent[position] // parts).reshape([-1 if axis == position else 1 for axis in range(len(extent))])
    return gain


def normal_values(key, dims, scale, limit, cuts=(), dtype=jnp.bfloat16):
    values = scale * jax.random.normal(key, dims, jnp.float32)
    if cuts:
        values = values * shard_levels(key, dims, cuts, -0.22, 0.18)
    return jnp.clip(values, -limit, limit).astype(dtype)


def setup_inputs(seed: int = 0) -> dict:
    keys = jax.random.split(jax.random.key(seed), 6)
    return {
        "right_side": normal_values(keys[0], (Q, NX, NY, NZ * RHS), 3.0, 18.0, ((1, 16), (2, 2), (3, 8)), jnp.float32),
        "cell_coef": jnp.clip(jnp.exp(math.log(2.0) - 1.3862944 * jax.random.uniform(keys[1], (NX, NY, NZ), jnp.float32) ** shard_levels(keys[1], (NX, NY, NZ), ((0, 16), (1, 2), (2, 8)), -0.2, 0.2)), 0.5, 2.0),
        "cell_matrix": draw_cell_matrix(jax.random.fold_in(keys[5], 71), 0),
        "face_coupling": normal_values(keys[3], (3, Q, Q), 0.03, 0.18, (), jnp.float32),
        "patch_inverse": draw_patch_inverse(jax.random.fold_in(keys[5], 71), 0),
    }


HIGH = lax.Precision.HIGHEST

def operator(values, cell_coef, cell_matrix, face_coupling):
    result = cell_coef[None, :, :, :, None] * jnp.einsum('pq,qxyzr->pxyzr', cell_matrix, values, precision=HIGH)
    for direction in range(3):
        forward = jnp.roll(values, -1, direction + 1)
        behind = jnp.roll(values, 1, direction + 1)
        result = result - jnp.einsum('pq,qxyzr->pxyzr', face_coupling[direction], forward, precision=HIGH)
        result = result - jnp.einsum('qp,qxyzr->pxyzr', face_coupling[direction], behind, precision=HIGH)
    return result

def reference(right_side, cell_coef, cell_matrix, face_coupling, patch_inverse):
    dof_count = cell_matrix.shape[0]
    residual = right_side.reshape(dof_count, NX, NY, NZ, RHS)
    solution = jnp.zeros_like(residual)
    scaling = lax.rsqrt(cell_coef)[None, :, :, :, None]
    blocks = patch_inverse.astype(jnp.float32).reshape(dof_count, 2, 2, 2, dof_count, 2, 2, 2)
    for colour in range(8):
        shifts = (1 - colour // 4, 1 - colour // 2 % 2, 1 - colour % 2)
        scaled = (scaling * residual).astype(jnp.bfloat16)
        scaled = lax.optimization_barrier(scaled).astype(jnp.float32)
        rolled = jnp.roll(scaled, shifts, axis=(1, 2, 3))
        blocked = rolled.reshape(dof_count, NX // 2, 2, NY // 2, 2, NZ // 2, 2, RHS)
        solved = jnp.einsum('qijkplmn,pXlYmZnr->qXiYjZkr', blocks, blocked, precision=HIGH)
        solved = solved.reshape(dof_count, NX, NY, NZ, RHS)
        solved = jnp.roll(solved, (-shifts[0], -shifts[1], -shifts[2]), axis=(1, 2, 3))
        correction = scaling * solved
        solution = solution + correction
        residual = residual - operator(correction, cell_coef, cell_matrix, face_coupling)
    return (solution.reshape(right_side.shape), residual.reshape(right_side.shape))
```

```python
import functools

import jax
import jax.numpy as jnp
from jax import lax
from jax.experimental import pallas as pl
from jax.experimental.pallas import tpu as pltpu
from jax.sharding import PartitionSpec as P

Q = 81
F = 88
B = 96
L = 128
F32, BF16 = jnp.float32, jnp.bfloat16

SWAP, SINIT, SHIFT, PRE, POSTX, POSTZ, MID, OUTS, COPIES = 0, 1, 3, 5, 9, 17, 21, 23, 25


def padded(tile):
    return jnp.concatenate([tile, jnp.zeros((B - F, tile.shape[1]), F32)], axis=0).astype(BF16)


def roll(tile, shift):
    shift = shift % L
    return pltpu.roll(tile, shift, 1) if shift else tile


def kernel(
    nx, nz,
    b_ref, coef_ref, p_ref, w_ref,
    sol_ref, res_ref,
    perm, perm_back, stage, arrive, partner_in, R, S, SN, CF, SEP, SOM, su, sd, hsl, hsu,
    xs, xr, XK, OUT, CB, DB, YR, ZR, XL, XU, PU, PD, HL, HU, QU, QD, GL, GU, MS, MR, OIN, OS,
    send_sem, recv_sem,
):
    gx, gy, gz = lax.axis_index("gx"), lax.axis_index("gy"), lax.axis_index("gz")
    partner = (gx, 1 - gy, gz)
    x_up, x_down = (lax.rem(gx + 1, nx), gy, gz), (lax.rem(gx + nx - 1, nx), gy, gz)
    z_up, z_down = (gx, gy, lax.rem(gz + 1, nz)), (gx, gy, lax.rem(gz + nz - 1, nz))

    def copy(index, src, dst, device):
        return pltpu.make_async_remote_copy(
            src_ref=src, dst_ref=dst, send_sem=send_sem.at[index], recv_sem=recv_sem.at[index],
            device_id=device, device_id_type=pl.DeviceIdType.MESH,
        )

    barrier = pltpu.get_barrier_semaphore()
    for device in (partner, x_up, x_down, z_up, z_down):
        pl.semaphore_signal(barrier, inc=1, device_id=device, device_id_type=pl.DeviceIdType.MESH)

    lane = lax.broadcasted_iota(jnp.int32, (F, L), 1)
    zlane = lax.rem(lane, 16)
    first, last = zlane == 0, zlane == 15
    lane96 = lax.broadcasted_iota(jnp.int32, (B, L), 1)
    half96 = lane96 < 64
    lane8 = lax.broadcasted_iota(jnp.int32, (8, L), 1)
    zlane8 = lax.rem(lane8, 16)

    def source_of(n):
        r, zp, y, zq = n // 128, (n // 64) % 2, (n // 16) % 4, n % 16
        return y * 128 + (2 * zq + zp) * 4 + r

    rows = lax.broadcasted_iota(jnp.int32, (128, 512), 0)
    cols = lax.broadcasted_iota(jnp.int32, (128, 512), 1)
    for i in range(4):
        perm[128 * i : 128 * i + 128, :] = (rows + 128 * i == source_of(cols)).astype(F32).astype(BF16)
        perm_back[128 * i : 128 * i + 128, :] = (source_of(rows + 128 * i) == cols).astype(F32).astype(BF16)

    stage[...] = jnp.zeros_like(stage)
    S[...] = jnp.zeros_like(S)

    def enter(x, carry):
        for yp in range(2):
            for y in range(4):
                row = x * 8 + 2 * y + yp
                stage[0:Q, y * L : y * L + L] = b_ref[pl.ds(row, Q, 32), :]
                coef = coef_ref[pl.ds(row, 1), :]
                high = coef.astype(BF16).astype(F32)
                stage[Q : Q + 1, y * L : y * L + L] = high
                stage[Q + 1 : Q + 2, y * L : y * L + L] = coef - high
            sorted_ = jnp.dot(stage[...].astype(BF16), perm[...], preferred_element_type=F32)
            for r in range(4):
                arrive[r, x, yp] = sorted_[:, r * L : r * L + L].astype(BF16)
        return carry

    lax.fori_loop(0, 4, enter, 0)
    pl.semaphore_wait(barrier, 5)
    swap = copy(SWAP, arrive.at[pl.ds(2 * (1 - gy), 2)], partner_in, partner)
    swap.start()
    swap.wait()

    def gather(h, x, yp):
        own = arrive[2 * gy + h, x, yp].astype(F32)
        other = partner_in[h, x, yp].astype(F32)
        lo, hi = jnp.where(gy == 0, own, other), jnp.where(gy == 0, other, own)
        return jnp.where(half96, lo, roll(hi, 64)), jnp.where(half96, roll(lo, 64), hi)

    def keep_coef(xi, yp, zp, tile):
        coef = jnp.broadcast_to(tile[Q : Q + 1] + tile[Q + 1 : Q + 2], (8, L))
        CF[xi, yp, zp] = coef
        SN[xi, yp, zp] = lax.rsqrt(coef)

    shifts = [copy(SHIFT + h, xs.at[h], xr.at[h], x_up) for h in range(2)]
    for h in range(2):
        for yp in range(2):
            for zp, tile in enumerate(gather(h, 3, yp)):
                xs[h, yp, zp] = tile.astype(BF16)
                if h == 0:
                    keep_coef(4, yp, zp, tile)
        shifts[h].start()

    def place(x, carry):
        for h in range(2):
            for yp in range(2):
                for zp, tile in enumerate(gather(h, x, yp)):
                    R[h, x, yp, zp] = tile[:F]
                    if h == 0:
                        keep_coef(x + 1, yp, zp, tile)
        return carry

    lax.fori_loop(0, 3, place, 0)
    for h in range(2):
        shifts[h].wait()
        for yp in range(2):
            for zp in range(2):
                tile = xr[h, yp, zp].astype(F32)
                R[h, 3, yp, zp] = tile[:F]
                if h == 0:
                    keep_coef(0, yp, zp, tile)

    up, down = jnp.zeros((8, L), F32), jnp.zeros((8, L), F32)
    for xi in range(5):
        for yp in range(2):
            j = 2 * xi + yp
            up = jnp.where(zlane8 == j, roll(SN[xi, yp, 1], j - 15), up)
            down = jnp.where(zlane8 == j, roll(SN[xi, yp, 0], j), down)
    su[...] = up
    sd[...] = down
    s_copies = [copy(SINIT, su, hsl, z_up), copy(SINIT + 1, sd, hsu, z_down)]
    for c in s_copies:
        c.start()
    for c in s_copies:
        c.wait()
    for xi in range(5):
        for yp in range(2):
            j = 2 * xi + yp
            SEP[xi, yp] = jnp.where(zlane8 == 15, roll(hsu[...], 15 - j), roll(SN[xi, yp, 0], -1))
            SOM[xi, yp] = jnp.where(zlane8 == 0, roll(hsl[...], -j), roll(SN[xi, yp, 1], 1))

    def round_of_four(a, carry):
        def slot(l):
            return lax.rem(l + 3 * (1 - a), 4)

        def times(ref, index, tile):
            return ref[index][0:1] * tile

        mids = [copy(MID + h, MS.at[h], MR.at[h], x_down) for h in range(2)]

        @pl.when(a == 1)
        def _():
            for h in range(2):
                for yp in range(2):
                    for zp in range(2):
                        MS[h, 0, yp, zp] = padded(R[h, 3, yp, zp])
                        MS[h, 1, yp, zp] = padded(S[h, 3, yp, zp])
                mids[h].start()
            for h in range(2):
                mids[h].wait()
                for yp in range(2):
                    for zp in range(2):
                        R[h, 3, yp, zp] = MR[h, 0, yp, zp][:F].astype(F32)
                        S[h, 3, yp, zp] = MR[h, 1, yp, zp][:F].astype(F32)

        def pre_copies(h):
            return (
                copy(PRE + 2 * h, PU.at[h], HL.at[h], z_up),
                copy(PRE + 2 * h + 1, PD.at[h], HU.at[h], z_down),
            )

        def x_copies(h, g):
            return (
                copy(POSTX + 4 * h + 2 * g, CB.at[h, slot(3)], XL.at[h, g], x_up),
                copy(POSTX + 4 * h + 2 * g + 1, CB.at[h, slot(0)], XU.at[h, g], x_down),
            )

        def z_copies(h):
            return (
                copy(POSTZ + 2 * h, QU.at[h], GL.at[h], z_up),
                copy(POSTZ + 2 * h + 1, QD.at[h], GU.at[h], z_down),
            )

        def pre(h):
            up, down = jnp.zeros((F, L), F32), jnp.zeros((F, L), F32)
            for l in range(4):
                for yp in range(2):
                    j = 2 * l + yp
                    tile = times(SN, (l + a, yp, 1), R[h, slot(l), yp, 1])
                    up = jnp.where(zlane == j, roll(tile, j - 15), up)
                    tile = times(SN, (l + a, yp, 0), R[h, slot(l), yp, 0])
                    down = jnp.where(zlane == j, roll(tile, j), down)
            PU[h] = padded(up)
            PD[h] = padded(down)
            for c in pre_copies(h):
                c.start()

        def frames(b, g):
            for dx in range(2):
                for dy in range(2):
                    for dz in range(2):
                        yp, zp = (dy if b else 1 - dy), (dz if g else 1 - dz)
                        ry, rz = int(not b and dy == 0), int(not g and dz == 0)
                        yield 4 * dx + 2 * dy + dz, dx, yp, zp, ry, rz

        def solve(h, b, g):
            if g == 0:
                for c in pre_copies(h):
                    c.wait_recv()
            for k, dx, yp, zp, ry, rz in frames(b, g):
                for X in range(2):
                    l = 2 * X + dx
                    tile = times(SN, (l + a, yp, zp), R[h, slot(l), yp, zp])
                    tile = roll(tile, 16 * ry + rz)
                    if rz:
                        ghost = roll(HL[h].astype(F32)[:F], 16 * ry - (2 * l + yp))
                        tile = jnp.where(first, ghost, tile)
                    XK[k * B : k * B + B, X * L : X * L + L] = padded(tile)
                if g == 0:
                    edge = (PU if rz else HU)[h].astype(F32)
                    XK[k * B : k * B + B, 2 * L : 3 * L] = roll(edge, 16 * ry - (2 * dx + yp)).astype(BF16)
            width = 256 if g else 384
            OUT[:, :width] = jnp.dot(p_ref[...], XK[:, :width], preferred_element_type=F32)
            if g == 0:
                for c in pre_copies(h):
                    c.wait_send()
            up, down = jnp.zeros((F, L), F32), jnp.zeros((F, L), F32)
            for X in range(2):
                for k, dx, yp, zp, ry, rz in frames(b, g):
                    l = 2 * X + dx
                    j = 2 * l + yp
                    block = OUT[k * F : k * F + F, X * L : X * L + L]
                    if g:
                        corr = times(SN, (l + a, yp, zp), roll(block, -16 * ry))
                        if zp:
                            up = jnp.where(zlane == j, roll(corr, j - 15), up)
                            beside = roll(corr, 1)
                        else:
                            down = jnp.where(zlane == j, roll(corr, j), down)
                            beside = roll(corr, -1)
                    else:
                        edge = OUT[k * F : k * F + F, 2 * L : 3 * L]
                        here = roll(block, -16 * ry)
                        above = jnp.where(last, roll(edge, 15 - 4 * X - 16 * ry), roll(block, -16 * ry - 1))
                        if zp:
                            corr = times(SN, (l + a, yp, 1), above)
                            beside = times(SOM, (l + a, yp), here)
                        else:
                            corr = times(SN, (l + a, yp, 0), here)
                            beside = times(SEP, (l + a, yp), above)
                    S[h, slot(l), yp, zp] += corr
                    CB[h, slot(l), yp, zp] = padded(corr)
                    DB[h, slot(l), yp, zp] = padded(times(CF, (l + a, yp, zp), corr))
                    YR[h, slot(l), yp, zp] = padded(roll(corr, 16 if yp else -16))
                    ZR[h, slot(l), yp, zp] = padded(beside)
                x_copies(h, g)[1 - X].start()
            if g:
                QU[h] = padded(up)
                QD[h] = padded(down)
                for c in z_copies(h):
                    c.start()

        def update(h, g):
            if g:
                for c in z_copies(h):
                    c.wait_recv()
            for l in (1, 2, 0, 3):
                if l == 0:
                    x_copies(h, g)[0].wait_recv()
                if l == 3:
                    x_copies(h, g)[1].wait_recv()
                for yp in range(2):
                    s = slot(l)
                    j = 2 * l + yp
                    pair = lambda ref, *index: [ref[(*index, 0)], ref[(*index, 1)]]
                    own = pair(CB, h, s, yp)
                    behind, ahead = ZR[h, s, yp, 1], ZR[h, s, yp, 0]
                    if g:
                        ghost = roll(GL[h].astype(F32)[:F], -j)
                        behind = padded(jnp.where(first, ghost, behind.astype(F32)[:F]))
                        ghost = roll(GU[h].astype(F32)[:F], 15 - j)
                        ahead = padded(jnp.where(last, ghost, ahead.astype(F32)[:F]))
                    blocks = [
                        pair(DB, h, s, yp),
                        pair(CB, h, slot(l - 1), yp) if l else pair(XL, h, g, yp),
                        pair(CB, h, slot(l + 1), yp) if l < 3 else pair(XU, h, g, yp),
                        pair(CB, h, s, 0) if yp else pair(YR, h, s, 1),
                        pair(YR, h, s, 0) if yp else pair(CB, h, s, 1),
                        [behind, own[0]],
                        [own[1], ahead],
                    ]
                    stacked = jnp.concatenate([jnp.concatenate(block, axis=1) for block in blocks], axis=0)
                    change = jnp.dot(w_ref[...], stacked, preferred_element_type=F32)
                    R[h, s, yp, 0] -= change[:, :L]
                    R[h, s, yp, 1] -= change[:, L:]
            for c in x_copies(h, g) + (z_copies(h) if g else ()):
                c.wait_send()

        for h in range(2):
            pre(h)
        for b in range(2):
            for g in range(2):
                for h in range(2):
                    solve(h, b, g)
                for h in range(2):
                    update(h, g)
                    if g == 1 and b == 0:
                        pre(h)
        return carry

    lax.fori_loop(0, 2, round_of_four, 0)

    outs = [copy(OUTS + w, OS.at[w], OIN.at[w, pl.ds(2 * gy, 2)], partner) for w in range(2)]
    for w, field in enumerate((S, R)):

        def leave(x, carry):
            for h in range(2):
                for yp in range(2):
                    even, odd = field[h, x, yp, 0], field[h, x, yp, 1]
                    lo = jnp.where(lane < 64, even, roll(odd, 64))
                    hi = jnp.where(lane < 64, roll(even, 64), odd)
                    OIN[w, 2 * gy + h, x, yp] = padded(jnp.where(gy == 0, lo, hi))
                    OS[w, h, x, yp] = padded(jnp.where(gy == 0, hi, lo))
            return carry

        lax.fori_loop(0, 4, leave, 0)
        outs[w].start()
    for w, out_ref in enumerate((sol_ref, res_ref)):
        outs[w].wait()

        def finish(x, carry):
            for yp in range(2):
                tiles = jnp.concatenate([OIN[w, r, x, yp] for r in range(4)], axis=1)
                back = jnp.dot(tiles, perm_back[...], preferred_element_type=F32)
                for y in range(4):
                    out_ref[pl.ds(x * 8 + 2 * y + yp, Q, 32), :] = back[:Q, y * L : y * L + L]
            return carry

        lax.fori_loop(0, 4, finish, 0)


def on_device(nx, nz, right_side, cell_coef, cell_matrix, face_coupling, patch_inverse):
    flat = right_side.reshape(-1, L)
    coef = jnp.repeat(cell_coef, 4, axis=2).reshape(-1, L)
    blocks = patch_inverse.reshape(Q, 8, Q, 8).transpose(1, 0, 3, 2)
    blocks = jnp.pad(blocks, ((0, 0), (0, F - Q), (0, 0), (0, B - Q))).reshape(8 * F, 8 * B)
    parts = [cell_matrix]
    for d in range(3):
        parts += [-face_coupling[d].T, -face_coupling[d]]
    weights = jnp.concatenate([jnp.pad(p, ((0, F - Q), (0, B - Q))) for p in parts], axis=1).astype(BF16)
    tile = lambda *dims, t=BF16: pltpu.VMEM((*dims, B if t == BF16 else F, L), t)
    vmem = pl.BlockSpec(memory_space=pltpu.VMEM)
    sol, res = pl.pallas_call(
        functools.partial(kernel, nx, nz),
        out_shape=[jax.ShapeDtypeStruct(flat.shape, F32)] * 2,
        in_specs=[vmem] * 4,
        out_specs=[vmem] * 2,
        scratch_shapes=[
            pltpu.VMEM((512, 512), BF16),
            pltpu.VMEM((512, 512), BF16),
            pltpu.VMEM((B, 512), F32),
            tile(4, 4, 2),
            tile(2, 4, 2),
            tile(2, 4, 2, 2, t=F32),
            tile(2, 4, 2, 2, t=F32),
            pltpu.VMEM((5, 2, 2, 8, L), F32),
            pltpu.VMEM((5, 2, 2, 8, L), F32),
            pltpu.VMEM((5, 2, 8, L), F32),
            pltpu.VMEM((5, 2, 8, L), F32),
            *[pltpu.VMEM((8, L), F32)] * 4,
            tile(2, 2, 2), tile(2, 2, 2),
            pltpu.VMEM((8 * B, 3 * L), BF16),
            pltpu.VMEM((8 * F, 3 * L), F32),
            *[tile(2, 4, 2, 2)] * 4,
            *[tile(2, 2, 2, 2)] * 2,
            *[tile(2)] * 8,
            *[tile(2, 2, 2, 2)] * 2,
            tile(2, 4, 4, 2),
            tile(2, 2, 4, 2),
            pltpu.SemaphoreType.DMA((COPIES,)),
            pltpu.SemaphoreType.DMA((COPIES,)),
        ],
        compiler_params=pltpu.CompilerParams(
            collective_id=0, has_side_effects=True, vmem_limit_bytes=60 * 1024 * 1024
        ),
    )(flat, coef, blocks, weights)
    return sol.reshape(right_side.shape), res.reshape(right_side.shape)


def solution(mesh):
    fields = P(None, "gx", "gy", "gz")
    return jax.shard_map(
        functools.partial(on_device, mesh.shape["gx"], mesh.shape["gz"]),
        mesh=mesh,
        in_specs=(fields, P("gx", "gy", "gz"), P(), P(), P()),
        out_specs=(fields, fields),
        check_vma=False,
    )
```

```python
import functools

import jax
import jax.numpy as jnp
from jax import lax
from jax.experimental import pallas as pl
from jax.experimental.pallas import tpu as pltpu
from jax.sharding import PartitionSpec as P

Q = 81
F = 88
B = 96
L = 128
F32, BF16 = jnp.float32, jnp.bfloat16
MESH = pl.DeviceIdType.MESH

SWAP, SINIT, SHIFT, PRE, POSTX, POSTZ, MID, OUTS, COPIES = 0, 1, 3, 5, 9, 17, 21, 25, 29


def padded(tile):
    return jnp.concatenate([tile, jnp.zeros((B - F, tile.shape[1]), F32)], axis=0).astype(BF16)


def roll(tile, shift):
    shift = shift % L
    return pltpu.roll(tile, shift, 1) if shift else tile


def one_hot(shape, hit):
    rows = lax.broadcasted_iota(jnp.int32, shape, 0)
    cols = lax.broadcasted_iota(jnp.int32, shape, 1)
    return jnp.where(hit(rows, cols), 1.0, 0.0).astype(BF16)


def source_of(n):
    return ((n >> 4) & 3) * 128 + (n & 15) * 8 + ((n >> 6) & 1) * 4 + (n >> 7)


def kernel(
    nx, nz,
    b_ref, coef_ref, p_ref, m_ref, f_ref,
    out_ref,
    perm, stage, coefs, p_rows, p_cols, p_stack, PINV, square, W,
    arrive, partner_in, R, S, SN, CF, SEP, SOM, su, sd, hsl, hsu,
    xr, XK, OUT, CB, DB, YR, ZR, XL, XU, PU, PD, HL, HU, QU, QD, GL, GU, MS, MR, OIN, OS,
    send_sem, recv_sem, out_sem,
):
    gx, gy, gz = lax.axis_index("gx"), lax.axis_index("gy"), lax.axis_index("gz")
    up_x, down_x = lax.rem(gx + 1, nx), lax.rem(gx + nx - 1, nx)
    partner = (gx, 1 - gy, gz)
    x_up, x_down = (up_x, gy, gz), (down_x, gy, gz)
    z_up, z_down = (gx, gy, lax.rem(gz + 1, nz)), (gx, gy, lax.rem(gz + nz - 1, nz))
    cross_up, cross_down = (up_x, 1 - gy, gz), (down_x, 1 - gy, gz)

    def copy(index, src, dst, device):
        return pltpu.make_async_remote_copy(
            src_ref=src, dst_ref=dst, send_sem=send_sem.at[index], recv_sem=recv_sem.at[index],
            device_id=device, device_id_type=MESH,
        )

    barrier = pltpu.get_barrier_semaphore()
    for device in (partner, x_up, x_down, z_up, z_down, cross_up, cross_down):
        pl.semaphore_signal(barrier, inc=1, device_id=device, device_id_type=MESH)

    lane = lax.broadcasted_iota(jnp.int32, (F, L), 1)
    zlane = lane & 15
    first, last = zlane == 0, zlane == 15
    half96 = lax.broadcasted_iota(jnp.int32, (B, L), 1) < 64
    zlane8 = lax.broadcasted_iota(jnp.int32, (8, L), 1) & 15

    perm[...] = one_hot((512, 512), lambda r, c: r == source_of(c))
    spread = one_hot((32, L), lambda r, c: r == (c >> 2))
    coef = coef_ref[...]
    high = coef.astype(BF16)
    low = (coef - high.astype(F32)).astype(BF16)
    coefs[0] = jnp.dot(high, spread, preferred_element_type=F32)
    coefs[1] = jnp.dot(low, spread, preferred_element_type=F32)
    stage[...] = jnp.zeros_like(stage)

    def enter(x):
        for yp in range(2):
            for y in range(4):
                row = x * 8 + 2 * y + yp
                stage[0:Q, y * L : y * L + L] = b_ref[pl.ds(row, Q, 32), :]
                stage[Q : Q + 1, y * L : y * L + L] = coefs[0, pl.ds(row, 1), :]
                stage[Q + 1 : Q + 2, y * L : y * L + L] = coefs[1, pl.ds(row, 1), :]
            ordered = jnp.dot(stage[...].astype(BF16), perm[...], preferred_element_type=F32)
            for r in range(4):
                arrive[r, x, yp] = ordered[:, r * L : r * L + L].astype(BF16)

    enter(3)
    pl.semaphore_wait(barrier, 7)
    shifts = [
        copy(SHIFT, arrive.at[pl.ds(2 * gy, 2), 3], xr.at[0], x_up),
        copy(SHIFT + 1, arrive.at[pl.ds(2 * (1 - gy), 2), 3], xr.at[1], cross_up),
    ]
    for c in shifts:
        c.start()

    def enter_rest(x, carry):
        enter(x)
        return carry

    lax.fori_loop(0, 3, enter_rest, 0)
    swap = copy(SWAP, arrive.at[pl.ds(2 * (1 - gy), 2)], partner_in, partner)
    swap.start()

    for i in range(6):
        chunk = p_ref[:, i * L : min(i * L + L, 8 * Q)].astype(F32)
        short = L - chunk.shape[1]
        if short:
            chunk = jnp.concatenate([chunk, jnp.zeros((8 * Q, short), F32)], axis=1)
        p_rows[i] = chunk
    for o in range(8):
        for i in range(6):
            rows = p_rows[i, pl.ds(o, Q, 8), :]
            rows = jnp.concatenate([rows, jnp.zeros((F - Q, L), F32)], axis=0)
            p_stack[o * F : o * F + F, i * L : i * L + L] = rows.astype(BF16)
    for i in range(6):
        p_cols[128 * i : 128 * i + 128, :] = one_hot(
            (128, 8 * B), lambda r, c: r + 128 * i == 8 * (c - 96 * ((c * 683) >> 16)) + ((c * 683) >> 16)
        )
    PINV[...] = jnp.dot(p_stack[...], p_cols[...], preferred_element_type=F32).astype(BF16)
    square[...] = jnp.zeros_like(square)
    weights = jnp.zeros((F, 7 * B), F32)
    for i in range(4):
        square[0:Q, 0:Q] = f_ref[i - 1] if i else m_ref[...]
        whole = square[...]
        parts = [(0, whole)] if i == 0 else [(2 * i - 1, -whole.T), (2 * i, -whole)]
        for at, part in parts:
            place = one_hot((L, 7 * B), lambda r, c: (r + B * at == c) & (r < B))
            weights += jnp.dot(part[:F].astype(BF16), place, preferred_element_type=F32)
    W[...] = weights.astype(BF16)
    S[...] = jnp.zeros_like(S)

    def joined(own, other):
        own, other = own.astype(F32), other.astype(F32)
        lo, hi = jnp.where(gy == 0, own, other), jnp.where(gy == 0, other, own)
        return jnp.where(half96, lo, roll(hi, 64)), jnp.where(half96, roll(lo, 64), hi)

    def keep_coef(xi, yp, zp, tile):
        value = jnp.broadcast_to(tile[Q : Q + 1] + tile[Q + 1 : Q + 2], (8, L))
        CF[xi, yp, zp] = value
        SN[xi, yp, zp] = lax.rsqrt(value)

    swap.wait()

    def place(x, carry):
        for h in range(2):
            for yp in range(2):
                for zp, tile in enumerate(joined(arrive[2 * gy + h, x, yp], partner_in[h, x, yp])):
                    R[h, x, yp, zp] = tile[:F]
                    if h == 0:
                        keep_coef(x + 1, yp, zp, tile)
        return carry

    lax.fori_loop(0, 4, place, 0)
    for c in shifts:
        c.wait()
    for h in range(2):
        for yp in range(2):
            for zp, tile in enumerate(joined(xr[0, h, yp], xr[1, h, yp])):
                R[h, 3, yp, zp] = tile[:F]
                if h == 0:
                    keep_coef(0, yp, zp, tile)

    up, down = jnp.zeros((8, L), F32), jnp.zeros((8, L), F32)
    for xi in range(5):
        for yp in range(2):
            j = 2 * xi + yp
            up = jnp.where(zlane8 == j, roll(SN[xi, yp, 1], j - 15), up)
            down = jnp.where(zlane8 == j, roll(SN[xi, yp, 0], j), down)
    su[...] = up
    sd[...] = down
    s_copies = [copy(SINIT, su, hsl, z_up), copy(SINIT + 1, sd, hsu, z_down)]
    for c in s_copies:
        c.start()

    def slot(l, a):
        return (l + 3 * (1 - a)) % 4 if isinstance(a, int) else lax.rem(l + 3 * (1 - a), 4)

    def times(ref, index, tile):
        return ref[index][0:1] * tile

    def pre_copies(h):
        return (
            copy(PRE + 2 * h, PU.at[h], HL.at[h], z_up),
            copy(PRE + 2 * h + 1, PD.at[h], HU.at[h], z_down),
        )

    def x_copy(h, g, a, way):
        if way:
            return copy(POSTX + 4 * h + 2 * g + 1, CB.at[h, slot(0, a)], XU.at[h, g], x_down)
        return copy(POSTX + 4 * h + 2 * g, CB.at[h, slot(3, a)], XL.at[h, g], x_up)

    def z_copies(h):
        return (
            copy(POSTZ + 2 * h, QU.at[h], GL.at[h], z_up),
            copy(POSTZ + 2 * h + 1, QD.at[h], GU.at[h], z_down),
        )

    def mid_copy(h, which):
        return copy(MID + 2 * h + which, MS.at[h, which], MR.at[h, which], x_down)

    def out_copy(w, h):
        return copy(OUTS + 2 * w + h, OS.at[w, h], OIN.at[w, 2 * gy + h], partner)

    def pre(h, a):
        up, down = jnp.zeros((F, L), F32), jnp.zeros((F, L), F32)
        for l in range(4):
            for yp in range(2):
                j = 2 * l + yp
                tile = times(SN, (l + a, yp, 1), R[h, slot(l, a), yp, 1])
                up = jnp.where(zlane == j, roll(tile, j - 15), up)
                tile = times(SN, (l + a, yp, 0), R[h, slot(l, a), yp, 0])
                down = jnp.where(zlane == j, roll(tile, j), down)
        PU[h] = padded(up)
        PD[h] = padded(down)
        for c in pre_copies(h):
            c.start()

    def frames(b, g):
        for dx in range(2):
            for dy in range(2):
                for dz in range(2):
                    yp, zp = (dy if b else 1 - dy), (dz if g else 1 - dz)
                    ry, rz = int(not b and dy == 0), int(not g and dz == 0)
                    yield 4 * dx + 2 * dy + dz, dx, yp, zp, ry, rz

    def solve(h, a, b, g):
        if g == 0:
            for c in pre_copies(h):
                c.wait_recv()
        for k, dx, yp, zp, ry, rz in frames(b, g):
            for X in range(2):
                l = 2 * X + dx
                tile = times(SN, (l + a, yp, zp), R[h, slot(l, a), yp, zp])
                tile = roll(tile, 16 * ry + rz)
                if rz:
                    ghost = roll(HL[h].astype(F32)[:F], 16 * ry - (2 * l + yp))
                    tile = jnp.where(first, ghost, tile)
                XK[k * B : k * B + B, X * L : X * L + L] = padded(tile)
            if g == 0:
                edge = (PU if rz else HU)[h].astype(F32)
                XK[k * B : k * B + B, 2 * L : 3 * L] = roll(edge, 16 * ry - (2 * dx + yp)).astype(BF16)
        width = 256 if g else 384
        OUT[:, :width] = jnp.dot(PINV[...], XK[:, :width], preferred_element_type=F32)
        if g == 0:
            for c in pre_copies(h):
                c.wait_send()
        up, down = jnp.zeros((F, L), F32), jnp.zeros((F, L), F32)
        for X in range(2):
            for k, dx, yp, zp, ry, rz in frames(b, g):
                l = 2 * X + dx
                j = 2 * l + yp
                s = slot(l, a)
                block = OUT[k * F : k * F + F, X * L : X * L + L]
                if g:
                    corr = times(SN, (l + a, yp, zp), roll(block, -16 * ry))
                    if zp:
                        up = jnp.where(zlane == j, roll(corr, j - 15), up)
                        beside = roll(corr, 1)
                    else:
                        down = jnp.where(zlane == j, roll(corr, j), down)
                        beside = roll(corr, -1)
                else:
                    edge = OUT[k * F : k * F + F, 2 * L : 3 * L]
                    here = roll(block, -16 * ry)
                    above = jnp.where(last, roll(edge, 15 - 4 * X - 16 * ry), roll(block, -16 * ry - 1))
                    if zp:
                        corr = times(SN, (l + a, yp, 1), above)
                        beside = times(SOM, (l + a, yp), here)
                    else:
                        corr = times(SN, (l + a, yp, 0), here)
                        beside = times(SEP, (l + a, yp), above)
                S[h, s, yp, zp] += corr
                CB[h, s, yp, zp] = padded(corr)
                DB[h, s, yp, zp] = padded(times(CF, (l + a, yp, zp), corr))
                YR[h, s, yp, zp] = padded(roll(corr, 16 if yp else -16))
                ZR[h, s, yp, zp] = padded(beside)
            x_copy(h, g, a, 1 - X).start()
        if g:
            QU[h] = padded(up)
            QD[h] = padded(down)
            for c in z_copies(h):
                c.start()

    def update(h, a, g):
        if g:
            for c in z_copies(h):
                c.wait_recv()
        for l in (1, 2, 0, 3):
            if l == 0:
                x_copy(h, g, a, 0).wait_recv()
            if l == 3:
                x_copy(h, g, a, 1).wait_recv()
            s = slot(l, a)
            for yp in range(2):
                j = 2 * l + yp
                pair = lambda ref, *index: [ref[(*index, 0)], ref[(*index, 1)]]
                own = pair(CB, h, s, yp)
                behind, ahead = ZR[h, s, yp, 1], ZR[h, s, yp, 0]
                if g:
                    ghost = roll(GL[h].astype(F32)[:F], -j)
                    behind = padded(jnp.where(first, ghost, behind.astype(F32)[:F]))
                    ghost = roll(GU[h].astype(F32)[:F], 15 - j)
                    ahead = padded(jnp.where(last, ghost, ahead.astype(F32)[:F]))
                blocks = [
                    pair(DB, h, s, yp),
                    pair(CB, h, slot(l - 1, a), yp) if l else pair(XL, h, g, yp),
                    pair(CB, h, slot(l + 1, a), yp) if l < 3 else pair(XU, h, g, yp),
                    pair(CB, h, s, 0) if yp else pair(YR, h, s, 1),
                    pair(YR, h, s, 0) if yp else pair(CB, h, s, 1),
                    [behind, own[0]],
                    [own[1], ahead],
                ]
                stacked = jnp.concatenate([jnp.concatenate(block, axis=1) for block in blocks], axis=0)
                change = jnp.dot(W[...], stacked, preferred_element_type=F32)
                R[h, s, yp, 0] -= change[:, :L]
                R[h, s, yp, 1] -= change[:, L:]
        for c in (x_copy(h, g, a, 0), x_copy(h, g, a, 1)) + (z_copies(h) if g else ()):
            c.wait_send()

    def leave(w, h, field):
        def one(x, carry):
            for yp in range(2):
                even, odd = field[h, x, yp, 0], field[h, x, yp, 1]
                lo = jnp.where(lane < 64, even, roll(odd, 64))
                hi = jnp.where(lane < 64, roll(even, 64), odd)
                OIN[w, 2 * gy + h, x, yp] = padded(jnp.where(gy == 0, lo, hi))
                OS[w, h, x, yp] = padded(jnp.where(gy == 0, hi, lo))
            return carry

        lax.fori_loop(0, 4, one, 0)
        out_copy(w, h).start()

    for h in range(2):
        pre(h, 0)
    for c in s_copies:
        c.wait()
    for xi in range(5):
        for yp in range(2):
            j = 2 * xi + yp
            SEP[xi, yp] = jnp.where(zlane8 == 15, roll(hsu[...], 15 - j), roll(SN[xi, yp, 0], -1))
            SOM[xi, yp] = jnp.where(zlane8 == 0, roll(hsl[...], -j), roll(SN[xi, yp, 1], 1))

    def round_of_four(a, carry):
        for b in range(2):
            for h in range(2):
                solve(h, a, b, 0)
            for h in range(2):
                update(h, a, 0)
                solve(h, a, b, 1)
            if b == 0:
                for h in range(2):
                    update(h, a, 1)
                    pre(h, a)

        @pl.when(a == 1)
        def _():
            for h in range(2):
                mid_copy(h, 1).wait()
                for yp in range(2):
                    for zp in range(2):
                        S[h, 3, yp, zp] += MR[h, 1, yp, zp][:F].astype(F32)
                leave(0, h, S)

        for h in range(2):
            update(h, a, 1)

            @pl.when(a == 0)
            def _():
                for which, field in enumerate((R, S)):
                    for yp in range(2):
                        for zp in range(2):
                            MS[h, which, yp, zp] = padded(field[h, 3, yp, zp])
                    mid_copy(h, which).start()
                S[h, 3] = jnp.zeros((2, 2, F, L), F32)

        @pl.when(a == 0)
        def _():
            for h in range(2):
                mid_copy(h, 0).wait()
                for yp in range(2):
                    for zp in range(2):
                        R[h, 3, yp, zp] = MR[h, 0, yp, zp][:F].astype(F32)
                pre(h, 1)

        return carry

    lax.fori_loop(0, 2, round_of_four, 0)
    for h in range(2):
        leave(1, h, R)
    stores = [pltpu.make_async_copy(OIN.at[w], out_ref.at[w], out_sem.at[w]) for w in range(2)]
    for w in range(2):
        for h in range(2):
            out_copy(w, h).wait()
        stores[w].start()
    for c in stores:
        c.wait()


def finish(in_ref, sol_ref, res_ref, perm):
    perm[...] = one_hot((512, 512), lambda r, c: source_of(r) == c)
    for w, out_ref in enumerate((sol_ref, res_ref)):

        def one(x, carry):
            for yp in range(2):
                tiles = jnp.concatenate([in_ref[w, r, x, yp] for r in range(4)], axis=1)
                back = jnp.dot(tiles, perm[...], preferred_element_type=F32)
                for y in range(4):
                    out_ref[pl.ds(x * 8 + 2 * y + yp, Q, 32), :] = back[:Q, y * L : y * L + L]
            return carry

        lax.fori_loop(0, 4, one, 0)


def on_device(nx, nz, right_side, cell_coef, cell_matrix, face_coupling, patch_inverse):
    flat = right_side.reshape(-1, L)
    tile = lambda *dims, t=BF16: pltpu.VMEM((*dims, B if t == BF16 else F, L), t)
    vmem = pl.BlockSpec(memory_space=pltpu.VMEM)
    ordered = pl.pallas_call(
        functools.partial(kernel, nx, nz),
        out_shape=jax.ShapeDtypeStruct((2, 4, 4, 2, B, L), BF16),
        in_specs=[vmem] * 5,
        out_specs=pl.BlockSpec(memory_space=pl.ANY),
        scratch_shapes=[
            pltpu.VMEM((512, 512), BF16),
            pltpu.VMEM((B, 512), F32),
            pltpu.VMEM((2, 32, L), F32),
            pltpu.VMEM((6, 8 * Q, L), F32),
            pltpu.VMEM((8 * B, 8 * B), BF16),
            pltpu.VMEM((8 * F, 8 * B), BF16),
            pltpu.VMEM((8 * F, 8 * B), BF16),
            pltpu.VMEM((L, L), F32),
            pltpu.VMEM((F, 7 * B), BF16),
            tile(4, 4, 2),
            tile(2, 4, 2),
            tile(2, 4, 2, 2, t=F32),
            tile(2, 4, 2, 2, t=F32),
            pltpu.VMEM((5, 2, 2, 8, L), F32),
            pltpu.VMEM((5, 2, 2, 8, L), F32),
            pltpu.VMEM((5, 2, 8, L), F32),
            pltpu.VMEM((5, 2, 8, L), F32),
            *[pltpu.VMEM((8, L), F32)] * 4,
            tile(2, 2, 2),
            pltpu.VMEM((8 * B, 3 * L), BF16),
            pltpu.VMEM((8 * F, 3 * L), F32),
            *[tile(2, 4, 2, 2)] * 4,
            *[tile(2, 2, 2, 2)] * 2,
            *[tile(2)] * 8,
            *[tile(2, 2, 2, 2)] * 2,
            tile(2, 4, 4, 2),
            tile(2, 2, 4, 2),
            pltpu.SemaphoreType.DMA((COPIES,)),
            pltpu.SemaphoreType.DMA((COPIES,)),
            pltpu.SemaphoreType.DMA((2,)),
        ],
        compiler_params=pltpu.CompilerParams(
            collective_id=0, has_side_effects=True, vmem_limit_bytes=48 * 1024 * 1024
        ),
    )(flat, cell_coef.reshape(32, 32), patch_inverse, cell_matrix, face_coupling)
    sol, res = pl.pallas_call(
        finish,
        out_shape=[jax.ShapeDtypeStruct(flat.shape, F32)] * 2,
        in_specs=[vmem],
        out_specs=[vmem] * 2,
        scratch_shapes=[pltpu.VMEM((512, 512), BF16)],
    )(ordered)
    return sol.reshape(right_side.shape), res.reshape(right_side.shape)


def solution(mesh):
    fields = P(None, "gx", "gy", "gz")
    return jax.shard_map(
        functools.partial(on_device, mesh.shape["gx"], mesh.shape["gz"]),
        mesh=mesh,
        in_specs=(fields, P("gx", "gy", "gz"), P(), P(), P()),
        out_specs=(fields, fields),
        check_vma=False,
    )
```

```python
import functools

import jax
import jax.numpy as jnp
from jax import lax
from jax.experimental import pallas as pl
from jax.experimental.pallas import tpu as pltpu
from jax.sharding import PartitionSpec as P

Q = 81
F = 88
B = 96
L = 128
F32, BF16 = jnp.float32, jnp.bfloat16
MESH = pl.DeviceIdType.MESH

SWAP, SINIT, SHIFT, PRE, POSTX, POSTZ, MID, OUTS, SLANT, COPIES = 0, 1, 3, 5, 9, 17, 21, 25, 29, 33


def padded(tile):
    return jnp.concatenate([tile, jnp.zeros((B - F, tile.shape[1]), F32)], axis=0).astype(BF16)


def roll(tile, shift):
    shift = shift % L
    return pltpu.roll(tile, shift, 1) if shift else tile


def one_hot(shape, hit):
    rows = lax.broadcasted_iota(jnp.int32, shape, 0)
    cols = lax.broadcasted_iota(jnp.int32, shape, 1)
    return jnp.where(hit(rows, cols), 1.0, 0.0).astype(BF16)


def source_of(n):
    return ((n >> 4) & 3) * 128 + (n & 15) * 8 + ((n >> 6) & 1) * 4 + (n >> 7)


def kernel(
    nx, nz,
    b_any, coef_any, p_any, m_any, f_any,
    out_ref,
    b_ref, coef_ref, p_ref, m_ref, f_ref, perm, stage, coefs, p_rows, p_cols, p_stack, PINV, square, W, W_LOW, W_HIGH, W_BELOW, W_ABOVE,
    arrive, partner_in, R, S, SN, CF, SEP, SOM, su, sd, hsl, hsu,
    xr, XK, OUT, CB, DB, YR, ZR, XL, XU, PU, PD, HL, HU, QU, QD, GL, GU, HLX, HUX, MS, MR, OIN, OS,
    send_sem, recv_sem, load_sem, out_sem,
):
    gx, gy, gz = lax.axis_index("gx"), lax.axis_index("gy"), lax.axis_index("gz")
    up_x, down_x = lax.rem(gx + 1, nx), lax.rem(gx + nx - 1, nx)
    partner = (gx, 1 - gy, gz)
    x_up, x_down = (up_x, gy, gz), (down_x, gy, gz)
    z_up, z_down = (gx, gy, lax.rem(gz + 1, nz)), (gx, gy, lax.rem(gz + nz - 1, nz))
    cross_up, cross_down = (up_x, 1 - gy, gz), (down_x, 1 - gy, gz)

    def copy(index, src, dst, device):
        return pltpu.make_async_remote_copy(
            src_ref=src, dst_ref=dst, send_sem=send_sem.at[index], recv_sem=recv_sem.at[index],
            device_id=device, device_id_type=MESH,
        )

    loads = [
        pltpu.make_async_copy(src, dst, load_sem.at[i])
        for i, (src, dst) in enumerate(
            ((coef_any, coef_ref), (b_any, b_ref), (p_any, p_ref), (m_any, m_ref), (f_any, f_ref))
        )
    ]
    for c in loads:
        c.start()
    slant_up, slant_down = (down_x, gy, z_up[2]), (down_x, gy, z_down[2])
    barrier = pltpu.get_barrier_semaphore()
    for device in (
        partner, x_up, x_down, z_up, z_down, cross_up, cross_down,
        slant_up, slant_down, (up_x, gy, z_up[2]), (up_x, gy, z_down[2]),
    ):
        pl.semaphore_signal(barrier, inc=1, device_id=device, device_id_type=MESH)

    lane = lax.broadcasted_iota(jnp.int32, (F, L), 1)
    zlane = lane & 15
    first, last = zlane == 0, zlane == 15
    half96 = lax.broadcasted_iota(jnp.int32, (B, L), 1) < 64
    zlane8 = lax.broadcasted_iota(jnp.int32, (8, L), 1) & 15

    perm[...] = one_hot((512, 512), lambda r, c: r == source_of(c))
    spread = one_hot((32, L), lambda r, c: r == (c >> 2))
    loads[0].wait()
    coef = coef_ref[...]
    high = coef.astype(BF16)
    low = (coef - high.astype(F32)).astype(BF16)
    coefs[0] = jnp.dot(high, spread, preferred_element_type=F32)
    coefs[1] = jnp.dot(low, spread, preferred_element_type=F32)
    stage[...] = jnp.zeros_like(stage)

    def enter(x):
        for yp in range(2):
            for y in range(4):
                row = x * 8 + 2 * y + yp
                stage[0:Q, y * L : y * L + L] = b_ref[pl.ds(row, Q, 32), :]
                stage[Q : Q + 1, y * L : y * L + L] = coefs[0, pl.ds(row, 1), :]
                stage[Q + 1 : Q + 2, y * L : y * L + L] = coefs[1, pl.ds(row, 1), :]
            ordered = jnp.dot(stage[...].astype(BF16), perm[...], preferred_element_type=F32)
            for r in range(4):
                arrive[r, x, yp] = ordered[:, r * L : r * L + L].astype(BF16)

    loads[1].wait()
    enter(3)
    pl.semaphore_wait(barrier, 11)
    shifts = [
        copy(SHIFT, arrive.at[pl.ds(2 * gy, 2), 3], xr.at[0], x_up),
        copy(SHIFT + 1, arrive.at[pl.ds(2 * (1 - gy), 2), 3], xr.at[1], cross_up),
    ]
    for c in shifts:
        c.start()

    def enter_rest(x, carry):
        enter(x)
        return carry

    lax.fori_loop(0, 3, enter_rest, 0)
    swap = copy(SWAP, arrive.at[pl.ds(2 * (1 - gy), 2)], partner_in, partner)
    swap.start()

    for c in loads[2:]:
        c.wait()
    for i in range(6):
        chunk = p_ref[:, i * L : min(i * L + L, 8 * Q)].astype(F32)
        short = L - chunk.shape[1]
        if short:
            chunk = jnp.concatenate([chunk, jnp.zeros((8 * Q, short), F32)], axis=1)
        p_rows[i] = chunk
    for o in range(8):
        for i in range(6):
            rows = p_rows[i, pl.ds(o, Q, 8), :]
            rows = jnp.concatenate([rows, jnp.zeros((F - Q, L), F32)], axis=0)
            p_stack[o * F : o * F + F, i * L : i * L + L] = rows.astype(BF16)
    for i in range(6):
        p_cols[128 * i : 128 * i + 128, :] = one_hot(
            (128, 8 * B), lambda r, c: r + 128 * i == 8 * (c - 96 * ((c * 683) >> 16)) + ((c * 683) >> 16)
        )
    PINV[...] = jnp.dot(p_stack[...], p_cols[...], preferred_element_type=F32).astype(BF16)
    square[...] = jnp.zeros_like(square)
    weights = jnp.zeros((F, 7 * B), F32)
    for i in range(4):
        square[0:Q, 0:Q] = f_ref[i - 1] if i else m_ref[...]
        whole = square[...]
        below, above = (0, 6) if i == 1 else (2 * i - 2, 2 * i - 1)
        parts = [(1, whole)] if i == 0 else [(below, -whole.T), (above, -whole)]
        for at, part in parts:
            place = one_hot((L, 7 * B), lambda r, c: (r + B * at == c) & (r < B))
            weights += jnp.dot(part[:F].astype(BF16), place, preferred_element_type=F32)
    W[...] = weights.astype(BF16)
    W_LOW[...] = weights[:, B:].astype(BF16)
    W_HIGH[...] = weights[:, : 6 * B].astype(BF16)
    W_BELOW[...] = weights[:, :B].astype(BF16)
    W_ABOVE[...] = weights[:, 6 * B :].astype(BF16)
    S[...] = jnp.zeros_like(S)

    def joined(own, other):
        own, other = own.astype(F32), other.astype(F32)
        lo, hi = jnp.where(gy == 0, own, other), jnp.where(gy == 0, other, own)
        return jnp.where(half96, lo, roll(hi, 64)), jnp.where(half96, roll(lo, 64), hi)

    def keep_coef(xi, yp, zp, tile):
        value = jnp.broadcast_to(tile[Q : Q + 1] + tile[Q + 1 : Q + 2], (8, L))
        CF[xi, yp, zp] = value
        SN[xi, yp, zp] = lax.rsqrt(value)

    swap.wait()

    def place(x, carry):
        for h in range(2):
            for yp in range(2):
                for zp, tile in enumerate(joined(arrive[2 * gy + h, x, yp], partner_in[h, x, yp])):
                    R[h, x, yp, zp] = tile[:F]
                    if h == 0:
                        keep_coef(x + 1, yp, zp, tile)
        return carry

    lax.fori_loop(0, 4, place, 0)
    for c in shifts:
        c.wait()
    for h in range(2):
        for yp in range(2):
            for zp, tile in enumerate(joined(xr[0, h, yp], xr[1, h, yp])):
                R[h, 3, yp, zp] = tile[:F]
                if h == 0:
                    keep_coef(0, yp, zp, tile)

    up, down = jnp.zeros((8, L), F32), jnp.zeros((8, L), F32)
    for xi in range(5):
        for yp in range(2):
            j = 2 * xi + yp
            up = jnp.where(zlane8 == j, roll(SN[xi, yp, 1], j - 15), up)
            down = jnp.where(zlane8 == j, roll(SN[xi, yp, 0], j), down)
    su[...] = up
    sd[...] = down
    s_copies = [copy(SINIT, su, hsl, z_up), copy(SINIT + 1, sd, hsu, z_down)]
    for c in s_copies:
        c.start()

    def slot(l, a):
        return (l + 3 * (1 - a)) % 4 if isinstance(a, int) else lax.rem(l + 3 * (1 - a), 4)

    def times(ref, index, tile):
        return ref[index][0:1] * tile

    def pre_copies(h):
        return (
            copy(PRE + 2 * h, PU.at[h], HL.at[h], z_up),
            copy(PRE + 2 * h + 1, PD.at[h], HU.at[h], z_down),
        )

    def x_copy(h, g, a, way):
        if way:
            return copy(POSTX + 4 * h + 2 * g + 1, CB.at[h, slot(0, a)], XU.at[h, g], x_down)
        return copy(POSTX + 4 * h + 2 * g, CB.at[h, slot(3, a)], XL.at[h, g], x_up)

    def z_copies(h):
        return (
            copy(POSTZ + 2 * h, QU.at[h], GL.at[h], z_up),
            copy(POSTZ + 2 * h + 1, QD.at[h], GU.at[h], z_down),
        )

    def mid_copy(h, which):
        return copy(MID + 2 * h + which, MS.at[h, which], MR.at[h, which], x_down)

    def out_copy(w, h):
        return copy(OUTS + 2 * w + h, OS.at[w, h], OIN.at[w, 2 * gy + h], partner)

    def slant_copies(h):
        return (
            copy(SLANT + 2 * h, PU.at[h], HLX.at[h], slant_up),
            copy(SLANT + 2 * h + 1, PD.at[h], HUX.at[h], slant_down),
        )

    def pre(h, a):
        up, down = jnp.zeros((F, L), F32), jnp.zeros((F, L), F32)
        for l in range(4):
            for yp in range(2):
                j = 2 * l + yp
                tile = times(SN, (l + a, yp, 1), R[h, slot(l, a), yp, 1])
                up = jnp.where(zlane == j, roll(tile, j - 15), up)
                tile = times(SN, (l + a, yp, 0), R[h, slot(l, a), yp, 0])
                down = jnp.where(zlane == j, roll(tile, j), down)
        PU[h] = padded(up)
        PD[h] = padded(down)
        for c in pre_copies(h):
            c.start()

    def frames(b, g):
        for dx in range(2):
            for dy in range(2):
                for dz in range(2):
                    yp, zp = (dy if b else 1 - dy), (dz if g else 1 - dz)
                    ry, rz = int(not b and dy == 0), int(not g and dz == 0)
                    yield 4 * dx + 2 * dy + dz, dx, yp, zp, ry, rz

    def solve(h, a, b, g):
        for k, dx, yp, zp, ry, rz in frames(b, g):
            for X in range(2):
                l = 2 * X + dx
                tile = times(SN, (l + a, yp, zp), R[h, slot(l, a), yp, zp])
                tile = roll(tile, 16 * ry + rz)
                if rz:
                    ghost = roll(HL[h].astype(F32)[:F], 16 * ry - (2 * l + yp))
                    tile = jnp.where(first, ghost, tile)
                XK[k * B : k * B + B, X * L : X * L + L] = padded(tile)
            if g == 0:
                edge = (PU if rz else HU)[h].astype(F32)
                XK[k * B : k * B + B, 2 * L : 3 * L] = roll(edge, 16 * ry - (2 * dx + yp)).astype(BF16)
        width = 256 if g else 384
        OUT[:, :width] = jnp.dot(PINV[...], XK[:, :width], preferred_element_type=F32)
        up, down = jnp.zeros((F, L), F32), jnp.zeros((F, L), F32)
        for X, side in ((0, 0), (1, 1), (0, 1), (1, 0)):
            for k, dx, yp, zp, ry, rz in frames(b, g):
                if dx != side:
                    continue
                l = 2 * X + dx
                j = 2 * l + yp
                s = slot(l, a)
                block = OUT[k * F : k * F + F, X * L : X * L + L]
                if g:
                    corr = times(SN, (l + a, yp, zp), roll(block, -16 * ry))
                    if zp:
                        up = jnp.where(zlane == j, roll(corr, j - 15), up)
                        beside = roll(corr, 1)
                    else:
                        down = jnp.where(zlane == j, roll(corr, j), down)
                        beside = roll(corr, -1)
                else:
                    edge = OUT[k * F : k * F + F, 2 * L : 3 * L]
                    here = roll(block, -16 * ry)
                    above = jnp.where(last, roll(edge, 15 - 4 * X - 16 * ry), roll(block, -16 * ry - 1))
                    if zp:
                        corr = times(SN, (l + a, yp, 1), above)
                        beside = times(SOM, (l + a, yp), here)
                    else:
                        corr = times(SN, (l + a, yp, 0), here)
                        beside = times(SEP, (l + a, yp), above)
                S[h, s, yp, zp] += corr
                CB[h, s, yp, zp] = padded(corr)
                DB[h, s, yp, zp] = padded(times(CF, (l + a, yp, zp), corr))
                YR[h, s, yp, zp] = padded(roll(corr, 16 if yp else -16))
                ZR[h, s, yp, zp] = padded(beside)
            if X == side:
                x_copy(h, g, a, 1 - X).start()
        if g:
            QU[h] = padded(up)
            QD[h] = padded(down)
            for c in z_copies(h):
                c.start()

    def pair(ref, *index):
        return jnp.concatenate([ref[(*index, 0)], ref[(*index, 1)]], axis=1)

    def subtract(h, s, yp, weights, blocks):
        stacked = jnp.concatenate(blocks, axis=0) if len(blocks) > 1 else blocks[0]
        change = jnp.dot(weights[...], stacked, preferred_element_type=F32)
        R[h, s, yp, 0] -= change[:, :L]
        R[h, s, yp, 1] -= change[:, L:]

    def update(h, a, g):
        if g:
            for c in z_copies(h):
                c.wait_recv()
        for l in (0, 3, 1, 2):
            s = slot(l, a)
            for yp in range(2):
                j = 2 * l + yp
                even, odd = CB[h, s, yp, 0], CB[h, s, yp, 1]
                behind, ahead = ZR[h, s, yp, 1], ZR[h, s, yp, 0]
                if g:
                    ghost = roll(GL[h].astype(F32)[:F], -j)
                    behind = padded(jnp.where(first, ghost, behind.astype(F32)[:F]))
                    ghost = roll(GU[h].astype(F32)[:F], 15 - j)
                    ahead = padded(jnp.where(last, ghost, ahead.astype(F32)[:F]))
                blocks = [
                    pair(DB, h, s, yp),
                    pair(CB, h, s, 0) if yp else pair(YR, h, s, 1),
                    pair(YR, h, s, 0) if yp else pair(CB, h, s, 1),
                    jnp.concatenate([behind, even], axis=1),
                    jnp.concatenate([odd, ahead], axis=1),
                ]
                if l:
                    blocks = [pair(CB, h, slot(l - 1, a), yp)] + blocks
                if l < 3:
                    blocks = blocks + [pair(CB, h, slot(l + 1, a), yp)]
                subtract(h, s, yp, {0: W_LOW, 3: W_HIGH}.get(l, W), blocks)
        for way, (l, ghost, weights) in enumerate(((3, XL, W_BELOW), (0, XU, W_ABOVE))):
            x_copy(h, g, a, way).wait_recv()
            for yp in range(2):
                subtract(h, slot(3 - l, a), yp, weights, [pair(ghost, h, g, yp)])
        for c in (x_copy(h, g, a, 0), x_copy(h, g, a, 1)) + (z_copies(h) if g else ()):
            c.wait_send()

    def leave(w, h, field):
        def one(x, carry):
            for yp in range(2):
                even, odd = field[h, x, yp, 0], field[h, x, yp, 1]
                lo = jnp.where(lane < 64, even, roll(odd, 64))
                hi = jnp.where(lane < 64, roll(even, 64), odd)
                OIN[w, 2 * gy + h, x, yp] = padded(jnp.where(gy == 0, lo, hi))
                OS[w, h, x, yp] = padded(jnp.where(gy == 0, hi, lo))
            return carry

        lax.fori_loop(0, 4, one, 0)
        out_copy(w, h).start()

    for h in range(2):
        pre(h, 0)
    for c in s_copies:
        c.wait()
    for xi in range(5):
        for yp in range(2):
            j = 2 * xi + yp
            SEP[xi, yp] = jnp.where(zlane8 == 15, roll(hsu[...], 15 - j), roll(SN[xi, yp, 0], -1))
            SOM[xi, yp] = jnp.where(zlane8 == 0, roll(hsl[...], -j), roll(SN[xi, yp, 1], 1))

    def round_of_four(a, carry):
        for b in range(2):
            for h in range(2):
                if b:
                    for c in pre_copies(h):
                        c.wait()
                else:

                    @pl.when(a == 0)
                    def _():
                        for c in pre_copies(h):
                            c.wait()

                solve(h, a, b, 0)
            for h in range(2):
                update(h, a, 0)
                solve(h, a, b, 1)
            if b == 0:
                for h in range(2):
                    update(h, a, 1)
                    pre(h, a)

        @pl.when(a == 1)
        def _():
            for h in range(2):
                mid_copy(h, 1).wait()
                for yp in range(2):
                    for zp in range(2):
                        S[h, 3, yp, zp] += MR[h, 1, yp, zp][:F].astype(F32)
                leave(0, h, S)

        for h in range(2):
            update(h, a, 1)

            @pl.when(a == 0)
            def _():
                for which, field in enumerate((R, S)):
                    for yp in range(2):
                        for zp in range(2):
                            MS[h, which, yp, zp] = padded(field[h, 3, yp, zp])
                    mid_copy(h, which).start()
                    if which == 0:
                        pre(h, 0)
                        for c in slant_copies(h):
                            c.start()
                S[h, 3] = jnp.zeros((2, 2, F, L), F32)

        @pl.when(a == 0)
        def _():
            for h in range(2):
                mid_copy(h, 0).wait()
                top = jnp.zeros((F, L), F32)
                for yp in range(2):
                    for zp in range(2):
                        R[h, 3, yp, zp] = MR[h, 0, yp, zp][:F].astype(F32)
                    tile = times(SN, (4, yp, 1), MR[h, 0, yp, 1][:F].astype(F32))
                    top = jnp.where(zlane == 6 + yp, roll(tile, yp - 9), top)
                for c in pre_copies(h) + slant_copies(h):
                    c.wait()
                for edge, upper in ((HL, HLX[h].astype(F32)[:F]), (HU, HUX[h].astype(F32)[:F]), (PU, None)):
                    lower = roll(edge[h].astype(F32)[:F], -2)
                    upper = top if upper is None else roll(upper, 6)
                    edge[h] = padded(jnp.where(zlane < 6, lower, jnp.where(zlane < 8, upper, 0.0)))

        return carry

    lax.fori_loop(0, 2, round_of_four, 0)
    for h in range(2):
        leave(1, h, R)
    stores = [pltpu.make_async_copy(OIN.at[w], out_ref.at[w], out_sem.at[w]) for w in range(2)]
    for w in range(2):
        for h in range(2):
            out_copy(w, h).wait()
        stores[w].start()
    for c in stores:
        c.wait()


def finish(in_any, sol_any, res_any, in_ref, sol_ref, res_ref, perm, in_sem, out_sem):
    loads = [pltpu.make_async_copy(in_any.at[w], in_ref.at[w], in_sem.at[w]) for w in range(2)]
    for c in loads:
        c.start()
    perm[...] = one_hot((512, 512), lambda r, c: source_of(r) == c)
    outs = ((sol_ref, sol_any), (res_ref, res_any))
    stores = [pltpu.make_async_copy(src, dst, out_sem.at[w]) for w, (src, dst) in enumerate(outs)]
    for w, (out_ref, _) in enumerate(outs):
        loads[w].wait()

        def one(x, carry):
            tiles = jnp.concatenate(
                [jnp.concatenate([in_ref[w, r, x, yp] for r in range(4)], axis=1) for yp in range(2)], axis=0
            )
            back = jnp.dot(tiles, perm[...], preferred_element_type=F32)
            for yp in range(2):
                for y in range(4):
                    out_ref[pl.ds(x * 8 + 2 * y + yp, Q, 32), :] = back[yp * B : yp * B + Q, y * L : y * L + L]
            return carry

        lax.fori_loop(0, 4, one, 0)
        stores[w].start()
    for c in stores:
        c.wait()


def on_device(nx, nz, right_side, cell_coef, cell_matrix, face_coupling, patch_inverse):
    flat = right_side.reshape(-1, L)
    tile = lambda *dims, t=BF16: pltpu.VMEM((*dims, B if t == BF16 else F, L), t)
    whole = pl.BlockSpec(memory_space=pl.ANY)
    ordered = pl.pallas_call(
        functools.partial(kernel, nx, nz),
        out_shape=jax.ShapeDtypeStruct((2, 4, 4, 2, B, L), BF16),
        in_specs=[whole] * 5,
        out_specs=whole,
        scratch_shapes=[
            pltpu.VMEM(flat.shape, F32),
            pltpu.VMEM((32, 32), F32),
            pltpu.VMEM((8 * Q, 8 * Q), BF16),
            pltpu.VMEM((Q, Q), F32),
            pltpu.VMEM((3, Q, Q), F32),
            pltpu.VMEM((512, 512), BF16),
            pltpu.VMEM((B, 512), F32),
            pltpu.VMEM((2, 32, L), F32),
            pltpu.VMEM((6, 8 * Q, L), F32),
            pltpu.VMEM((8 * B, 8 * B), BF16),
            pltpu.VMEM((8 * F, 8 * B), BF16),
            pltpu.VMEM((8 * F, 8 * B), BF16),
            pltpu.VMEM((L, L), F32),
            pltpu.VMEM((F, 7 * B), BF16),
            *[pltpu.VMEM((F, 6 * B), BF16)] * 2,
            *[pltpu.VMEM((F, B), BF16)] * 2,
            tile(4, 4, 2),
            tile(2, 4, 2),
            tile(2, 4, 2, 2, t=F32),
            tile(2, 4, 2, 2, t=F32),
            pltpu.VMEM((5, 2, 2, 8, L), F32),
            pltpu.VMEM((5, 2, 2, 8, L), F32),
            pltpu.VMEM((5, 2, 8, L), F32),
            pltpu.VMEM((5, 2, 8, L), F32),
            *[pltpu.VMEM((8, L), F32)] * 4,
            tile(2, 2, 2),
            pltpu.VMEM((8 * B, 3 * L), BF16),
            pltpu.VMEM((8 * F, 3 * L), F32),
            *[tile(2, 4, 2, 2)] * 4,
            *[tile(2, 2, 2, 2)] * 2,
            *[tile(2)] * 10,
            *[tile(2, 2, 2, 2)] * 2,
            tile(2, 4, 4, 2),
            tile(2, 2, 4, 2),
            pltpu.SemaphoreType.DMA((COPIES,)),
            pltpu.SemaphoreType.DMA((COPIES,)),
            pltpu.SemaphoreType.DMA((5,)),
            pltpu.SemaphoreType.DMA((2,)),
        ],
        compiler_params=pltpu.CompilerParams(
            collective_id=0, has_side_effects=True, vmem_limit_bytes=67043328
        ),
    )(flat, cell_coef.reshape(32, 32), patch_inverse, cell_matrix, face_coupling)
    sol, res = pl.pallas_call(
        finish,
        out_shape=[jax.ShapeDtypeStruct(flat.shape, F32)] * 2,
        in_specs=[whole],
        out_specs=[whole] * 2,
        scratch_shapes=[
            tile(2, 4, 4, 2),
            *[pltpu.VMEM(flat.shape, F32)] * 2,
            pltpu.VMEM((512, 512), BF16),
            pltpu.SemaphoreType.DMA((2,)),
            pltpu.SemaphoreType.DMA((2,)),
        ],
        compiler_params=pltpu.CompilerParams(vmem_limit_bytes=67043328),
    )(ordered)
    return sol.reshape(right_side.shape), res.reshape(right_side.shape)


def solution(mesh):
    fields = P(None, "gx", "gy", "gz")
    return jax.shard_map(
        functools.partial(on_device, mesh.shape["gx"], mesh.shape["gz"]),
        mesh=mesh,
        in_specs=(fields, P("gx", "gy", "gz"), P(), P(), P()),
        out_specs=(fields, fields),
        check_vma=False,
    )
```

```python
import functools

import jax
import jax.numpy as jnp
from jax import lax
from jax.experimental import pallas as pl
from jax.experimental.pallas import tpu as pltpu
from jax.sharding import PartitionSpec as P

Q = 81
F = 88
B = 96
L = 128
F32, BF16 = jnp.float32, jnp.bfloat16
MESH = pl.DeviceIdType.MESH

SWAP, SINIT, SHIFT, PRE, POSTX, POSTZ, MID, OUTS, SLANT, RISE, SRISE, COPIES = 0, 1, 3, 5, 9, 17, 21, 25, 29, 33, 37, 39


def padded(tile):
    return jnp.concatenate([tile, jnp.zeros((B - F, tile.shape[1]), F32)], axis=0).astype(BF16)


def roll(tile, shift):
    shift = shift % L
    return pltpu.roll(tile, shift, 1) if shift else tile


def one_hot(shape, hit):
    rows = lax.broadcasted_iota(jnp.int32, shape, 0)
    cols = lax.broadcasted_iota(jnp.int32, shape, 1)
    return jnp.where(hit(rows, cols), 1.0, 0.0).astype(BF16)


def source_of(n):
    return ((n >> 4) & 3) * 128 + (n & 15) * 8 + ((n >> 6) & 1) * 4 + (n >> 7)


def kernel(
    nx, nz,
    b_any, coef_any, p_any, m_any, f_any,
    out_ref,
    b_ref, coef_ref, p_ref, m_ref, f_ref, perm, stage, coefs, p_rows, p_cols, p_stack, PINV, square, W, W_LOW, W_HIGH, W_BELOW, W_ABOVE,
    arrive, partner_in, R, S, SN, CF, SEP, SOM, su, sd, hsl, hsu, hslx, hsux,
    xr, XK, OUT, CB, DB, YR, ZR, XL, XU, PU, PD, HL, HU, QU, QD, GL, GU, HLX, HUX, MS, MR, OIN, OS,
    send_sem, recv_sem, load_sem, out_sem,
):
    gx, gy, gz = lax.axis_index("gx"), lax.axis_index("gy"), lax.axis_index("gz")
    up_x, down_x = lax.rem(gx + 1, nx), lax.rem(gx + nx - 1, nx)
    partner = (gx, 1 - gy, gz)
    x_up, x_down = (up_x, gy, gz), (down_x, gy, gz)
    z_up, z_down = (gx, gy, lax.rem(gz + 1, nz)), (gx, gy, lax.rem(gz + nz - 1, nz))
    cross_up, cross_down = (up_x, 1 - gy, gz), (down_x, 1 - gy, gz)

    def copy(index, src, dst, device):
        return pltpu.make_async_remote_copy(
            src_ref=src, dst_ref=dst, send_sem=send_sem.at[index], recv_sem=recv_sem.at[index],
            device_id=device, device_id_type=MESH,
        )

    loads = [
        pltpu.make_async_copy(src, dst, load_sem.at[i])
        for i, (src, dst) in enumerate(
            ((coef_any, coef_ref), (b_any, b_ref), (p_any, p_ref), (m_any, m_ref), (f_any, f_ref))
        )
    ]
    for c in loads:
        c.start()
    slant_up, slant_down = (down_x, gy, z_up[2]), (down_x, gy, z_down[2])
    barrier = pltpu.get_barrier_semaphore()
    for device in (
        partner, x_up, x_down, z_up, z_down, cross_up, cross_down,
        slant_up, slant_down, (up_x, gy, z_up[2]), (up_x, gy, z_down[2]),
    ):
        pl.semaphore_signal(barrier, inc=1, device_id=device, device_id_type=MESH)

    lane = lax.broadcasted_iota(jnp.int32, (F, L), 1)
    zlane = lane & 15
    first, last = zlane == 0, zlane == 15
    half96 = lax.broadcasted_iota(jnp.int32, (B, L), 1) < 64
    zlane8 = lax.broadcasted_iota(jnp.int32, (8, L), 1) & 15

    perm[...] = one_hot((512, 512), lambda r, c: r == source_of(c))
    spread = one_hot((32, L), lambda r, c: r == (c >> 2))
    loads[0].wait()
    coef = coef_ref[...]
    high = coef.astype(BF16)
    low = (coef - high.astype(F32)).astype(BF16)
    coefs[0] = jnp.dot(high, spread, preferred_element_type=F32)
    coefs[1] = jnp.dot(low, spread, preferred_element_type=F32)
    stage[...] = jnp.zeros_like(stage)

    def enter(x):
        for yp in range(2):
            for y in range(4):
                row = x * 8 + 2 * y + yp
                stage[0:Q, y * L : y * L + L] = b_ref[pl.ds(row, Q, 32), :]
                stage[Q : Q + 1, y * L : y * L + L] = coefs[0, pl.ds(row, 1), :]
                stage[Q + 1 : Q + 2, y * L : y * L + L] = coefs[1, pl.ds(row, 1), :]
            ordered = jnp.dot(stage[...].astype(BF16), perm[...], preferred_element_type=F32)
            for r in range(4):
                arrive[r, x, yp] = ordered[:, r * L : r * L + L].astype(BF16)

    loads[1].wait()
    enter(3)
    pl.semaphore_wait(barrier, 11)
    shifts = [
        copy(SHIFT, arrive.at[pl.ds(2 * gy, 2), 3], xr.at[0], x_up),
        copy(SHIFT + 1, arrive.at[pl.ds(2 * (1 - gy), 2), 3], xr.at[1], cross_up),
    ]
    for c in shifts:
        c.start()

    def enter_rest(x, carry):
        enter(x)
        return carry

    lax.fori_loop(0, 3, enter_rest, 0)
    swap = copy(SWAP, arrive.at[pl.ds(2 * (1 - gy), 2)], partner_in, partner)
    swap.start()

    for c in loads[2:]:
        c.wait()
    for i in range(6):
        chunk = p_ref[:, i * L : min(i * L + L, 8 * Q)].astype(F32)
        short = L - chunk.shape[1]
        if short:
            chunk = jnp.concatenate([chunk, jnp.zeros((8 * Q, short), F32)], axis=1)
        p_rows[i] = chunk
    for o in range(8):
        for i in range(6):
            rows = p_rows[i, pl.ds(o, Q, 8), :]
            rows = jnp.concatenate([rows, jnp.zeros((F - Q, L), F32)], axis=0)
            p_stack[o * F : o * F + F, i * L : i * L + L] = rows.astype(BF16)
    for i in range(6):
        p_cols[128 * i : 128 * i + 128, :] = one_hot(
            (128, 8 * B), lambda r, c: r + 128 * i == 8 * (c - 96 * ((c * 683) >> 16)) + ((c * 683) >> 16)
        )
    PINV[...] = jnp.dot(p_stack[...], p_cols[...], preferred_element_type=F32).astype(BF16)
    square[...] = jnp.zeros_like(square)
    weights = jnp.zeros((F, 7 * B), F32)
    for i in range(4):
        square[0:Q, 0:Q] = f_ref[i - 1] if i else m_ref[...]
        whole = square[...]
        below, above = (0, 6) if i == 1 else (2 * i - 2, 2 * i - 1)
        parts = [(1, whole)] if i == 0 else [(below, -whole.T), (above, -whole)]
        for at, part in parts:
            place = one_hot((L, 7 * B), lambda r, c: (r + B * at == c) & (r < B))
            weights += jnp.dot(part[:F].astype(BF16), place, preferred_element_type=F32)
    W[...] = weights.astype(BF16)
    W_LOW[...] = weights[:, B:].astype(BF16)
    W_HIGH[...] = weights[:, : 6 * B].astype(BF16)
    W_BELOW[...] = weights[:, :B].astype(BF16)
    W_ABOVE[...] = weights[:, 6 * B :].astype(BF16)
    S[...] = jnp.zeros_like(S)

    def joined(own, other):
        own, other = own.astype(F32), other.astype(F32)
        lo, hi = jnp.where(gy == 0, own, other), jnp.where(gy == 0, other, own)
        return jnp.where(half96, lo, roll(hi, 64)), jnp.where(half96, roll(lo, 64), hi)

    def keep_coef(xi, yp, zp, tile):
        value = jnp.broadcast_to(tile[Q : Q + 1] + tile[Q + 1 : Q + 2], (8, L))
        CF[xi, yp, zp] = value
        SN[xi, yp, zp] = lax.rsqrt(value)

    swap.wait()

    def place(x, carry):
        for h in range(2):
            for yp in range(2):
                for zp, tile in enumerate(joined(arrive[2 * gy + h, x, yp], partner_in[h, x, yp])):
                    R[h, x, yp, zp] = tile[:F]
                    if h == 0:
                        keep_coef(x + 1, yp, zp, tile)
        return carry

    lax.fori_loop(0, 4, place, 0)
    def slot(l, a):
        return (l + 3 * (1 - a)) % 4 if isinstance(a, int) else lax.rem(l + 3 * (1 - a), 4)

    def times(ref, index, tile):
        return ref[index][0:1] * tile

    def pre_copies(h):
        return (
            copy(PRE + 2 * h, PU.at[h], HL.at[h], z_up),
            copy(PRE + 2 * h + 1, PD.at[h], HU.at[h], z_down),
        )

    def x_copy(h, g, a, way):
        if way:
            return copy(POSTX + 4 * h + 2 * g + 1, CB.at[h, slot(0, a)], XU.at[h, g], x_down)
        return copy(POSTX + 4 * h + 2 * g, CB.at[h, slot(3, a)], XL.at[h, g], x_up)

    def z_copies(h):
        return (
            copy(POSTZ + 2 * h, QU.at[h], GL.at[h], z_up),
            copy(POSTZ + 2 * h + 1, QD.at[h], GU.at[h], z_down),
        )

    def mid_copy(h, which):
        return copy(MID + 2 * h + which, MS.at[h, which], MR.at[h, which], x_down)

    def out_copy(w, h):
        return copy(OUTS + 2 * w + h, OS.at[w, h], OIN.at[w, 2 * gy + h], partner)

    def slant_copies(h):
        return (
            copy(SLANT + 2 * h, PU.at[h], HLX.at[h], slant_up),
            copy(SLANT + 2 * h + 1, PD.at[h], HUX.at[h], slant_down),
        )

    def pre(h, a):
        up, down = jnp.zeros((F, L), F32), jnp.zeros((F, L), F32)
        for l in range(4):
            for yp in range(2):
                j = 2 * l + yp
                tile = times(SN, (l + a, yp, 1), R[h, slot(l, a), yp, 1])
                up = jnp.where(zlane == j, roll(tile, j - 15), up)
                tile = times(SN, (l + a, yp, 0), R[h, slot(l, a), yp, 0])
                down = jnp.where(zlane == j, roll(tile, j), down)
        PU[h] = padded(up)
        PD[h] = padded(down)
        for c in pre_copies(h):
            c.start()

    def frames(b, g):
        for dx in range(2):
            for dy in range(2):
                for dz in range(2):
                    yp, zp = (dy if b else 1 - dy), (dz if g else 1 - dz)
                    ry, rz = int(not b and dy == 0), int(not g and dz == 0)
                    yield 4 * dx + 2 * dy + dz, dx, yp, zp, ry, rz

    def solve(h, a, b, g):
        for k, dx, yp, zp, ry, rz in frames(b, g):
            for X in range(2):
                l = 2 * X + dx
                tile = times(SN, (l + a, yp, zp), R[h, slot(l, a), yp, zp])
                tile = roll(tile, 16 * ry + rz)
                if rz:
                    ghost = roll(HL[h].astype(F32)[:F], 16 * ry - (2 * l + yp))
                    tile = jnp.where(first, ghost, tile)
                XK[k * B : k * B + B, X * L : X * L + L] = padded(tile)
            if g == 0:
                edge = (PU if rz else HU)[h].astype(F32)
                XK[k * B : k * B + B, 2 * L : 3 * L] = roll(edge, 16 * ry - (2 * dx + yp)).astype(BF16)
        width = 256 if g else 384
        OUT[:, :width] = jnp.dot(PINV[...], XK[:, :width], preferred_element_type=F32)
        up, down = jnp.zeros((F, L), F32), jnp.zeros((F, L), F32)
        for X, side in ((0, 0), (1, 1), (0, 1), (1, 0)):
            for k, dx, yp, zp, ry, rz in frames(b, g):
                if dx != side:
                    continue
                l = 2 * X + dx
                j = 2 * l + yp
                s = slot(l, a)
                block = OUT[k * F : k * F + F, X * L : X * L + L]
                if g:
                    corr = times(SN, (l + a, yp, zp), roll(block, -16 * ry))
                    if zp:
                        up = jnp.where(zlane == j, roll(corr, j - 15), up)
                        beside = roll(corr, 1)
                    else:
                        down = jnp.where(zlane == j, roll(corr, j), down)
                        beside = roll(corr, -1)
                else:
                    edge = OUT[k * F : k * F + F, 2 * L : 3 * L]
                    here = roll(block, -16 * ry)
                    above = jnp.where(last, roll(edge, 15 - 4 * X - 16 * ry), roll(block, -16 * ry - 1))
                    if zp:
                        corr = times(SN, (l + a, yp, 1), above)
                        beside = times(SOM, (l + a, yp), here)
                    else:
                        corr = times(SN, (l + a, yp, 0), here)
                        beside = times(SEP, (l + a, yp), above)
                S[h, s, yp, zp] += corr
                CB[h, s, yp, zp] = padded(corr)
                DB[h, s, yp, zp] = padded(times(CF, (l + a, yp, zp), corr))
                YR[h, s, yp, zp] = padded(roll(corr, 16 if yp else -16))
                ZR[h, s, yp, zp] = padded(beside)
            if X == side:
                x_copy(h, g, a, 1 - X).start()
        if g:
            QU[h] = padded(up)
            QD[h] = padded(down)
            for c in z_copies(h):
                c.start()

    def pair(ref, *index):
        return jnp.concatenate([ref[(*index, 0)], ref[(*index, 1)]], axis=1)

    def subtract(h, s, yp, weights, blocks):
        stacked = jnp.concatenate(blocks, axis=0) if len(blocks) > 1 else blocks[0]
        change = jnp.dot(weights[...], stacked, preferred_element_type=F32)
        R[h, s, yp, 0] -= change[:, :L]
        R[h, s, yp, 1] -= change[:, L:]

    def update(h, a, g):
        if g:
            for c in z_copies(h):
                c.wait_recv()
        for l in (0, 3, 1, 2):
            s = slot(l, a)
            for yp in range(2):
                j = 2 * l + yp
                even, odd = CB[h, s, yp, 0], CB[h, s, yp, 1]
                behind, ahead = ZR[h, s, yp, 1], ZR[h, s, yp, 0]
                if g:
                    ghost = roll(GL[h].astype(F32)[:F], -j)
                    behind = padded(jnp.where(first, ghost, behind.astype(F32)[:F]))
                    ghost = roll(GU[h].astype(F32)[:F], 15 - j)
                    ahead = padded(jnp.where(last, ghost, ahead.astype(F32)[:F]))
                blocks = [
                    pair(DB, h, s, yp),
                    pair(CB, h, s, 0) if yp else pair(YR, h, s, 1),
                    pair(YR, h, s, 0) if yp else pair(CB, h, s, 1),
                    jnp.concatenate([behind, even], axis=1),
                    jnp.concatenate([odd, ahead], axis=1),
                ]
                if l:
                    blocks = [pair(CB, h, slot(l - 1, a), yp)] + blocks
                if l < 3:
                    blocks = blocks + [pair(CB, h, slot(l + 1, a), yp)]
                subtract(h, s, yp, {0: W_LOW, 3: W_HIGH}.get(l, W), blocks)
        for way, (l, ghost, weights) in enumerate(((3, XL, W_BELOW), (0, XU, W_ABOVE))):
            x_copy(h, g, a, way).wait_recv()
            for yp in range(2):
                subtract(h, slot(3 - l, a), yp, weights, [pair(ghost, h, g, yp)])
        for c in (x_copy(h, g, a, 0), x_copy(h, g, a, 1)) + (z_copies(h) if g else ()):
            c.wait_send()

    def leave(w, h, field):
        def one(x, carry):
            for yp in range(2):
                even, odd = field[h, x, yp, 0], field[h, x, yp, 1]
                lo = jnp.where(lane < 64, even, roll(odd, 64))
                hi = jnp.where(lane < 64, roll(even, 64), odd)
                OIN[w, 2 * gy + h, x, yp] = padded(jnp.where(gy == 0, lo, hi))
                OS[w, h, x, yp] = padded(jnp.where(gy == 0, hi, lo))
            return carry

        lax.fori_loop(0, 4, one, 0)
        out_copy(w, h).start()

    def each(body):
        def one(h, carry):
            body(h)
            return carry

        lax.fori_loop(0, 2, one, 0)

    rise_up, rise_down = (up_x, gy, z_up[2]), (up_x, gy, z_down[2])
    up, down = jnp.zeros((8, L), F32), jnp.zeros((8, L), F32)
    for xi in range(1, 5):
        for yp in range(2):
            j = 2 * xi + yp
            up = jnp.where(zlane8 == j, roll(SN[xi, yp, 1], j - 15), up)
            down = jnp.where(zlane8 == j, roll(SN[xi, yp, 0], j), down)
    su[...] = up
    sd[...] = down
    s_copies = [
        copy(SINIT, su, hsl, z_up), copy(SINIT + 1, sd, hsu, z_down),
        copy(SRISE, su, hslx, rise_up), copy(SRISE + 1, sd, hsux, rise_down),
    ]
    for c in s_copies:
        c.start()

    def rise_copies(h):
        return (
            copy(RISE + 2 * h, PU.at[h], HLX.at[h], rise_up),
            copy(RISE + 2 * h + 1, PD.at[h], HUX.at[h], rise_down),
        )

    def first_edges(h):
        pre(h, 1)
        for c in rise_copies(h):
            c.start()

    each(first_edges)
    for c in shifts:
        c.wait()
    for h in range(2):
        for yp in range(2):
            for zp, tile in enumerate(joined(xr[0, h, yp], xr[1, h, yp])):
                R[h, 3, yp, zp] = tile[:F]
                if h == 0:
                    keep_coef(0, yp, zp, tile)
    for c in s_copies:
        c.wait()
    for xi in range(5):
        for yp in range(2):
            lower, upper, j = (hsl, hsu, 2 * xi + yp) if xi else (hslx, hsux, 8 + yp)
            SEP[xi, yp] = jnp.where(zlane8 == 15, roll(upper[...], 15 - j), roll(SN[xi, yp, 0], -1))
            SOM[xi, yp] = jnp.where(zlane8 == 0, roll(lower[...], -j), roll(SN[xi, yp, 1], 1))

    def entry_edges(h):
        for c in pre_copies(h) + rise_copies(h):
            c.wait()
        low = jnp.zeros((F, L), F32)
        for yp in range(2):
            low = jnp.where(zlane == yp, roll(times(SN, (0, yp, 1), R[h, 3, yp, 1]), yp - 15), low)
        for edge, beyond in ((HL, HLX), (HU, HUX), (PU, None)):
            kept = roll(edge[h].astype(F32)[:F], 2)
            new = low if beyond is None else roll(beyond[h].astype(F32)[:F], -6)
            edge[h] = padded(jnp.where(zlane < 2, new, jnp.where(zlane < 8, kept, 0.0)))

    each(entry_edges)

    def round_of_four(a, carry):
        for b in range(2):

            def even(h):
                if b:
                    for c in pre_copies(h):
                        c.wait()
                solve(h, a, b, 0)

            def odd(h):
                update(h, a, 0)
                solve(h, a, b, 1)

            def between(h):
                update(h, a, 1)
                pre(h, a)

            each(even)
            each(odd)
            if b == 0:
                each(between)

        @pl.when(a == 1)
        def _():
            def add_shifted(h):
                mid_copy(h, 1).wait()
                for yp in range(2):
                    for zp in range(2):
                        S[h, 3, yp, zp] += MR[h, 1, yp, zp][:F].astype(F32)
                leave(0, h, S)

            each(add_shifted)

        def end(h):
            update(h, a, 1)

            @pl.when(a == 0)
            def _():
                for which, field in enumerate((R, S)):
                    for yp in range(2):
                        for zp in range(2):
                            MS[h, which, yp, zp] = padded(field[h, 3, yp, zp])
                    mid_copy(h, which).start()
                    if which == 0:
                        pre(h, 0)
                        for c in slant_copies(h):
                            c.start()
                S[h, 3] = jnp.zeros((2, 2, F, L), F32)

            @pl.when(a == 1)
            def _():
                leave(1, h, R)

        each(end)

        @pl.when(a == 0)
        def _():
            def shifted(h):
                mid_copy(h, 0).wait()
                top = jnp.zeros((F, L), F32)
                for yp in range(2):
                    for zp in range(2):
                        R[h, 3, yp, zp] = MR[h, 0, yp, zp][:F].astype(F32)
                    tile = times(SN, (4, yp, 1), MR[h, 0, yp, 1][:F].astype(F32))
                    top = jnp.where(zlane == 6 + yp, roll(tile, yp - 9), top)
                for c in pre_copies(h) + slant_copies(h):
                    c.wait()
                for edge, upper in ((HL, HLX[h].astype(F32)[:F]), (HU, HUX[h].astype(F32)[:F]), (PU, None)):
                    lower = roll(edge[h].astype(F32)[:F], -2)
                    upper = top if upper is None else roll(upper, 6)
                    edge[h] = padded(jnp.where(zlane < 6, lower, jnp.where(zlane < 8, upper, 0.0)))

            each(shifted)

        return carry

    lax.fori_loop(0, 2, round_of_four, 0)
    stores = [pltpu.make_async_copy(OIN.at[w], out_ref.at[w], out_sem.at[w]) for w in range(2)]
    for w in range(2):
        for h in range(2):
            out_copy(w, h).wait()
        stores[w].start()
    for c in stores:
        c.wait()


def finish(in_any, sol_any, res_any, in_ref, sol_ref, res_ref, perm, in_sem, out_sem):
    loads = [pltpu.make_async_copy(in_any.at[w], in_ref.at[w], in_sem.at[w]) for w in range(2)]
    for c in loads:
        c.start()
    perm[...] = one_hot((512, 512), lambda r, c: source_of(r) == c)
    outs = ((sol_ref, sol_any), (res_ref, res_any))
    stores = [pltpu.make_async_copy(src, dst, out_sem.at[w]) for w, (src, dst) in enumerate(outs)]
    for w, (out_ref, _) in enumerate(outs):
        loads[w].wait()

        def one(x, carry):
            tiles = jnp.concatenate(
                [jnp.concatenate([in_ref[w, r, x, yp] for r in range(4)], axis=1) for yp in range(2)], axis=0
            )
            back = jnp.dot(tiles, perm[...], preferred_element_type=F32)
            for yp in range(2):
                for y in range(4):
                    out_ref[pl.ds(x * 8 + 2 * y + yp, Q, 32), :] = back[yp * B : yp * B + Q, y * L : y * L + L]
            return carry

        lax.fori_loop(0, 4, one, 0)
        stores[w].start()
    for c in stores:
        c.wait()


def on_device(nx, nz, right_side, cell_coef, cell_matrix, face_coupling, patch_inverse):
    flat = right_side.reshape(-1, L)
    tile = lambda *dims, t=BF16: pltpu.VMEM((*dims, B if t == BF16 else F, L), t)
    whole = pl.BlockSpec(memory_space=pl.ANY)
    ordered = pl.pallas_call(
        functools.partial(kernel, nx, nz),
        out_shape=jax.ShapeDtypeStruct((2, 4, 4, 2, B, L), BF16),
        in_specs=[whole] * 5,
        out_specs=whole,
        scratch_shapes=[
            pltpu.VMEM(flat.shape, F32),
            pltpu.VMEM((32, 32), F32),
            pltpu.VMEM((8 * Q, 8 * Q), BF16),
            pltpu.VMEM((Q, Q), F32),
            pltpu.VMEM((3, Q, Q), F32),
            pltpu.VMEM((512, 512), BF16),
            pltpu.VMEM((B, 512), F32),
            pltpu.VMEM((2, 32, L), F32),
            pltpu.VMEM((6, 8 * Q, L), F32),
            pltpu.VMEM((8 * B, 8 * B), BF16),
            pltpu.VMEM((8 * F, 8 * B), BF16),
            pltpu.VMEM((8 * F, 8 * B), BF16),
            pltpu.VMEM((L, L), F32),
            pltpu.VMEM((F, 7 * B), BF16),
            *[pltpu.VMEM((F, 6 * B), BF16)] * 2,
            *[pltpu.VMEM((F, B), BF16)] * 2,
            tile(4, 4, 2),
            tile(2, 4, 2),
            tile(2, 4, 2, 2, t=F32),
            tile(2, 4, 2, 2, t=F32),
            pltpu.VMEM((5, 2, 2, 8, L), F32),
            pltpu.VMEM((5, 2, 2, 8, L), F32),
            pltpu.VMEM((5, 2, 8, L), F32),
            pltpu.VMEM((5, 2, 8, L), F32),
            *[pltpu.VMEM((8, L), F32)] * 6,
            tile(2, 2, 2),
            pltpu.VMEM((8 * B, 3 * L), BF16),
            pltpu.VMEM((8 * F, 3 * L), F32),
            *[tile(2, 4, 2, 2)] * 4,
            *[tile(2, 2, 2, 2)] * 2,
            *[tile(2)] * 10,
            *[tile(2, 2, 2, 2)] * 2,
            tile(2, 4, 4, 2),
            tile(2, 2, 4, 2),
            pltpu.SemaphoreType.DMA((COPIES,)),
            pltpu.SemaphoreType.DMA((COPIES,)),
            pltpu.SemaphoreType.DMA((5,)),
            pltpu.SemaphoreType.DMA((2,)),
        ],
        compiler_params=pltpu.CompilerParams(
            collective_id=0, has_side_effects=True, vmem_limit_bytes=67043328
        ),
    )(flat, cell_coef.reshape(32, 32), patch_inverse, cell_matrix, face_coupling)
    sol, res = pl.pallas_call(
        finish,
        out_shape=[jax.ShapeDtypeStruct(flat.shape, F32)] * 2,
        in_specs=[whole],
        out_specs=[whole] * 2,
        scratch_shapes=[
            tile(2, 4, 4, 2),
            *[pltpu.VMEM(flat.shape, F32)] * 2,
            pltpu.VMEM((512, 512), BF16),
            pltpu.SemaphoreType.DMA((2,)),
            pltpu.SemaphoreType.DMA((2,)),
        ],
        compiler_params=pltpu.CompilerParams(vmem_limit_bytes=67043328),
    )(ordered)
    return sol.reshape(right_side.shape), res.reshape(right_side.shape)


def solution(mesh):
    fields = P(None, "gx", "gy", "gz")
    return jax.shard_map(
        functools.partial(on_device, mesh.shape["gx"], mesh.shape["gz"]),
        mesh=mesh,
        in_specs=(fields, P("gx", "gy", "gz"), P(), P(), P()),
        out_specs=(fields, fields),
        check_vma=False,
    )
```

```python
import functools

import jax
import jax.numpy as jnp
from jax import lax
from jax.experimental import pallas as pl
from jax.experimental.pallas import tpu as pltpu
from jax.sharding import PartitionSpec as P

Q = 81
F = 88
B = 96
L = 128
PITCH = 40
F32, BF16 = jnp.float32, jnp.bfloat16
MESH = pl.DeviceIdType.MESH

SWAP, SINIT, SHIFT, PRE, POSTX, POSTZ, MID, OUTS, SLANT, RISE, SRISE, COPIES = 0, 1, 3, 5, 9, 17, 21, 25, 29, 33, 37, 39


def padded(tile):
    return jnp.concatenate([tile, jnp.zeros((B - F, tile.shape[1]), F32)], axis=0).astype(BF16)


def roll(tile, shift):
    shift = shift % L
    return pltpu.roll(tile, shift, 1) if shift else tile


def spaced(ref):
    return ref.reshape(Q, PITCH, L).at[:, :32, :]


def one_hot(shape, hit):
    rows = lax.broadcasted_iota(jnp.int32, shape, 0)
    cols = lax.broadcasted_iota(jnp.int32, shape, 1)
    return jnp.where(hit(rows, cols), 1.0, 0.0).astype(BF16)


def source_of(n):
    return ((n >> 4) & 3) * 128 + (n & 15) * 8 + ((n >> 6) & 1) * 4 + (n >> 7)


def kernel(
    nx, nz,
    b_any, coef_any, p_any, m_any, f_any,
    out_ref,
    b_ref, coef_ref, p_ref, m_ref, f_ref, perm, stage, coefs, p_rows, p_cols, p_stack, PINV, square, W, W_LOW, W_HIGH, W_BELOW, W_ABOVE,
    arrive, partner_in, R, S, SN, CF, SEP, SOM, su, sd, hsl, hsu, hslx, hsux,
    xr, XK, OUT, CB, DB, YR, ZR, XL, XU, PU, PD, HL, HU, QU, QD, GL, GU, HLX, HUX, MS, MR, OIN, OS,
    send_sem, recv_sem, load_sem, out_sem,
):
    gx, gy, gz = lax.axis_index("gx"), lax.axis_index("gy"), lax.axis_index("gz")
    up_x, down_x = lax.rem(gx + 1, nx), lax.rem(gx + nx - 1, nx)
    partner = (gx, 1 - gy, gz)
    x_up, x_down = (up_x, gy, gz), (down_x, gy, gz)
    z_up, z_down = (gx, gy, lax.rem(gz + 1, nz)), (gx, gy, lax.rem(gz + nz - 1, nz))
    cross_up, cross_down = (up_x, 1 - gy, gz), (down_x, 1 - gy, gz)

    def copy(index, src, dst, device):
        return pltpu.make_async_remote_copy(
            src_ref=src, dst_ref=dst, send_sem=send_sem.at[index], recv_sem=recv_sem.at[index],
            device_id=device, device_id_type=MESH,
        )

    loads = [
        pltpu.make_async_copy(src, dst, load_sem.at[i])
        for i, (src, dst) in enumerate(
            ((coef_any, coef_ref), (b_any, spaced(b_ref)), (p_any, p_ref), (m_any, m_ref), (f_any, f_ref))
        )
    ]
    for c in loads:
        c.start()
    slant_up, slant_down = (down_x, gy, z_up[2]), (down_x, gy, z_down[2])
    barrier = pltpu.get_barrier_semaphore()
    for device in (
        partner, x_up, x_down, z_up, z_down, cross_up, cross_down,
        slant_up, slant_down, (up_x, gy, z_up[2]), (up_x, gy, z_down[2]),
    ):
        pl.semaphore_signal(barrier, inc=1, device_id=device, device_id_type=MESH)

    lane = lax.broadcasted_iota(jnp.int32, (F, L), 1)
    zlane = lane & 15
    first, last = zlane == 0, zlane == 15
    half96 = lax.broadcasted_iota(jnp.int32, (B, L), 1) < 64
    zlane8 = lax.broadcasted_iota(jnp.int32, (8, L), 1) & 15

    perm[...] = one_hot((512, 512), lambda r, c: r == source_of(c))
    spread = one_hot((32, L), lambda r, c: r == (c >> 2))
    loads[0].wait()
    coef = coef_ref[...]
    high = coef.astype(BF16)
    low = (coef - high.astype(F32)).astype(BF16)
    coefs[0] = jnp.dot(high, spread, preferred_element_type=F32)
    coefs[1] = jnp.dot(low, spread, preferred_element_type=F32)
    stage[...] = jnp.zeros_like(stage)

    def enter(x):
        for yp in range(2):
            for y in range(4):
                row = x * 8 + 2 * y + yp
                stage[0:Q, y * L : y * L + L] = b_ref[pl.ds(row, Q, PITCH), :]
                stage[Q : Q + 1, y * L : y * L + L] = coefs[0, pl.ds(row, 1), :]
                stage[Q + 1 : Q + 2, y * L : y * L + L] = coefs[1, pl.ds(row, 1), :]
            ordered = jnp.dot(stage[...].astype(BF16), perm[...], preferred_element_type=F32)
            for r in range(4):
                arrive[r, x, yp] = ordered[:, r * L : r * L + L].astype(BF16)

    loads[1].wait()
    enter(3)
    pl.semaphore_wait(barrier, 11)
    shifts = [
        copy(SHIFT, arrive.at[pl.ds(2 * gy, 2), 3], xr.at[0], x_up),
        copy(SHIFT + 1, arrive.at[pl.ds(2 * (1 - gy), 2), 3], xr.at[1], cross_up),
    ]
    for c in shifts:
        c.start()

    def enter_rest(x, carry):
        enter(x)
        return carry

    lax.fori_loop(0, 3, enter_rest, 0)
    swap = copy(SWAP, arrive.at[pl.ds(2 * (1 - gy), 2)], partner_in, partner)
    swap.start()

    for c in loads[2:]:
        c.wait()
    for i in range(6):
        chunk = p_ref[:, i * L : min(i * L + L, 8 * Q)].astype(F32)
        short = L - chunk.shape[1]
        if short:
            chunk = jnp.concatenate([chunk, jnp.zeros((8 * Q, short), F32)], axis=1)
        p_rows[i] = chunk
    for o in range(8):
        for i in range(6):
            rows = p_rows[i, pl.ds(o, Q, 8), :]
            rows = jnp.concatenate([rows, jnp.zeros((F - Q, L), F32)], axis=0)
            p_stack[o * F : o * F + F, i * L : i * L + L] = rows.astype(BF16)
    for i in range(6):
        p_cols[128 * i : 128 * i + 128, :] = one_hot(
            (128, 8 * B), lambda r, c: r + 128 * i == 8 * (c - 96 * ((c * 683) >> 16)) + ((c * 683) >> 16)
        )
    PINV[...] = jnp.dot(p_stack[...], p_cols[...], preferred_element_type=F32).astype(BF16)
    square[...] = jnp.zeros_like(square)
    weights = jnp.zeros((F, 7 * B), F32)
    for i in range(4):
        square[0:Q, 0:Q] = f_ref[i - 1] if i else m_ref[...]
        whole = square[...]
        below, above = (0, 6) if i == 1 else (2 * i - 2, 2 * i - 1)
        parts = [(1, whole)] if i == 0 else [(below, -whole.T), (above, -whole)]
        for at, part in parts:
            place = one_hot((L, 7 * B), lambda r, c: (r + B * at == c) & (r < B))
            weights += jnp.dot(part[:F].astype(BF16), place, preferred_element_type=F32)
    W[...] = weights.astype(BF16)
    W_LOW[...] = weights[:, B:].astype(BF16)
    W_HIGH[...] = weights[:, : 6 * B].astype(BF16)
    W_BELOW[...] = weights[:, :B].astype(BF16)
    W_ABOVE[...] = weights[:, 6 * B :].astype(BF16)
    S[...] = jnp.zeros_like(S)

    def joined(own, other):
        own, other = own.astype(F32), other.astype(F32)
        lo, hi = jnp.where(gy == 0, own, other), jnp.where(gy == 0, other, own)
        return jnp.where(half96, lo, roll(hi, 64)), jnp.where(half96, roll(lo, 64), hi)

    def keep_coef(xi, yp, zp, tile):
        value = jnp.broadcast_to(tile[Q : Q + 1] + tile[Q + 1 : Q + 2], (8, L))
        CF[xi, yp, zp] = value
        SN[xi, yp, zp] = lax.rsqrt(value)

    swap.wait()

    def place(x, carry):
        for h in range(2):
            for yp in range(2):
                for zp, tile in enumerate(joined(arrive[2 * gy + h, x, yp], partner_in[h, x, yp])):
                    R[h, x, yp, zp] = tile[:F]
                    if h == 0:
                        keep_coef(x + 1, yp, zp, tile)
        return carry

    lax.fori_loop(0, 4, place, 0)
    def slot(l, a):
        return (l + 3 * (1 - a)) % 4 if isinstance(a, int) else lax.rem(l + 3 * (1 - a), 4)

    def times(ref, index, tile):
        return ref[index][0:1] * tile

    def pre_copies(h):
        return (
            copy(PRE + 2 * h, PU.at[h], HL.at[h], z_up),
            copy(PRE + 2 * h + 1, PD.at[h], HU.at[h], z_down),
        )

    def x_copy(h, g, a, way):
        if way:
            return copy(POSTX + 4 * h + 2 * g + 1, CB.at[h, slot(0, a)], XU.at[h, g], x_down)
        return copy(POSTX + 4 * h + 2 * g, CB.at[h, slot(3, a)], XL.at[h, g], x_up)

    def z_copies(h):
        return (
            copy(POSTZ + 2 * h, QU.at[h], GL.at[h], z_up),
            copy(POSTZ + 2 * h + 1, QD.at[h], GU.at[h], z_down),
        )

    def mid_copy(h, which):
        return copy(MID + 2 * h + which, MS.at[h, which], MR.at[h, which], x_down)

    def out_copy(w, h):
        return copy(OUTS + 2 * w + h, OS.at[w, h], OIN.at[w, 2 * gy + h], partner)

    def slant_copies(h):
        return (
            copy(SLANT + 2 * h, PU.at[h], HLX.at[h], slant_up),
            copy(SLANT + 2 * h + 1, PD.at[h], HUX.at[h], slant_down),
        )

    def pre(h, a):
        up, down = jnp.zeros((F, L), F32), jnp.zeros((F, L), F32)
        for l in range(4):
            for yp in range(2):
                j = 2 * l + yp
                tile = times(SN, (l + a, yp, 1), R[h, slot(l, a), yp, 1])
                up = jnp.where(zlane == j, roll(tile, j - 15), up)
                tile = times(SN, (l + a, yp, 0), R[h, slot(l, a), yp, 0])
                down = jnp.where(zlane == j, roll(tile, j), down)
        PU[h] = padded(up)
        PD[h] = padded(down)
        for c in pre_copies(h):
            c.start()

    def frames(b, g):
        for dx in range(2):
            for dy in range(2):
                for dz in range(2):
                    yp, zp = (dy if b else 1 - dy), (dz if g else 1 - dz)
                    ry, rz = int(not b and dy == 0), int(not g and dz == 0)
                    yield 4 * dx + 2 * dy + dz, dx, yp, zp, ry, rz

    def solve(h, a, b, g):
        for k, dx, yp, zp, ry, rz in frames(b, g):
            for X in range(2):
                l = 2 * X + dx
                tile = times(SN, (l + a, yp, zp), R[h, slot(l, a), yp, zp])
                tile = roll(tile, 16 * ry + rz)
                if rz:
                    ghost = roll(HL[h].astype(F32)[:F], 16 * ry - (2 * l + yp))
                    tile = jnp.where(first, ghost, tile)
                XK[k * B : k * B + B, X * L : X * L + L] = padded(tile)
            if g == 0:
                edge = (PU if rz else HU)[h].astype(F32)
                XK[k * B : k * B + B, 2 * L : 3 * L] = roll(edge, 16 * ry - (2 * dx + yp)).astype(BF16)
        width = 256 if g else 384
        OUT[:, :width] = jnp.dot(PINV[...], XK[:, :width], preferred_element_type=F32)
        up, down = jnp.zeros((F, L), F32), jnp.zeros((F, L), F32)
        for X, side in ((0, 0), (1, 1), (0, 1), (1, 0)):
            for k, dx, yp, zp, ry, rz in frames(b, g):
                if dx != side:
                    continue
                l = 2 * X + dx
                j = 2 * l + yp
                s = slot(l, a)
                block = OUT[k * F : k * F + F, X * L : X * L + L]
                if g:
                    corr = times(SN, (l + a, yp, zp), roll(block, -16 * ry))
                    if zp:
                        up = jnp.where(zlane == j, roll(corr, j - 15), up)
                        beside = roll(corr, 1)
                    else:
                        down = jnp.where(zlane == j, roll(corr, j), down)
                        beside = roll(corr, -1)
                else:
                    edge = OUT[k * F : k * F + F, 2 * L : 3 * L]
                    here = roll(block, -16 * ry)
                    above = jnp.where(last, roll(edge, 15 - 4 * X - 16 * ry), roll(block, -16 * ry - 1))
                    if zp:
                        corr = times(SN, (l + a, yp, 1), above)
                        beside = times(SOM, (l + a, yp), here)
                    else:
                        corr = times(SN, (l + a, yp, 0), here)
                        beside = times(SEP, (l + a, yp), above)
                S[h, s, yp, zp] += corr
                CB[h, s, yp, zp] = padded(corr)
                DB[h, s, yp, zp] = padded(times(CF, (l + a, yp, zp), corr))
                YR[h, s, yp, zp] = padded(roll(corr, 16 if yp else -16))
                ZR[h, s, yp, zp] = padded(beside)
            if X == side:
                x_copy(h, g, a, 1 - X).start()
        if g:
            QU[h] = padded(up)
            QD[h] = padded(down)
            for c in z_copies(h):
                c.start()

    def pair(ref, *index):
        return jnp.concatenate([ref[(*index, 0)], ref[(*index, 1)]], axis=1)

    def subtract(h, s, yp, weights, blocks):
        stacked = jnp.concatenate(blocks, axis=0) if len(blocks) > 1 else blocks[0]
        change = jnp.dot(weights[...], stacked, preferred_element_type=F32)
        R[h, s, yp, 0] -= change[:, :L]
        R[h, s, yp, 1] -= change[:, L:]

    def update(h, a, g):
        if g:
            for c in z_copies(h):
                c.wait_recv()
        for l in (0, 3, 1, 2):
            s = slot(l, a)
            for yp in range(2):
                j = 2 * l + yp
                even, odd = CB[h, s, yp, 0], CB[h, s, yp, 1]
                behind, ahead = ZR[h, s, yp, 1], ZR[h, s, yp, 0]
                if g:
                    ghost = roll(GL[h].astype(F32)[:F], -j)
                    behind = padded(jnp.where(first, ghost, behind.astype(F32)[:F]))
                    ghost = roll(GU[h].astype(F32)[:F], 15 - j)
                    ahead = padded(jnp.where(last, ghost, ahead.astype(F32)[:F]))
                blocks = [
                    pair(DB, h, s, yp),
                    pair(CB, h, s, 0) if yp else pair(YR, h, s, 1),
                    pair(YR, h, s, 0) if yp else pair(CB, h, s, 1),
                    jnp.concatenate([behind, even], axis=1),
                    jnp.concatenate([odd, ahead], axis=1),
                ]
                if l:
                    blocks = [pair(CB, h, slot(l - 1, a), yp)] + blocks
                if l < 3:
                    blocks = blocks + [pair(CB, h, slot(l + 1, a), yp)]
                subtract(h, s, yp, {0: W_LOW, 3: W_HIGH}.get(l, W), blocks)
        for way, (l, ghost, weights) in enumerate(((3, XL, W_BELOW), (0, XU, W_ABOVE))):
            x_copy(h, g, a, way).wait_recv()
            for yp in range(2):
                subtract(h, slot(3 - l, a), yp, weights, [pair(ghost, h, g, yp)])
        for c in (x_copy(h, g, a, 0), x_copy(h, g, a, 1)) + (z_copies(h) if g else ()):
            c.wait_send()

    def leave(w, h, field):
        def one(x, carry):
            for yp in range(2):
                even, odd = field[h, x, yp, 0], field[h, x, yp, 1]
                lo = jnp.where(lane < 64, even, roll(odd, 64))
                hi = jnp.where(lane < 64, roll(even, 64), odd)
                OIN[w, 2 * gy + h, x, yp] = padded(jnp.where(gy == 0, lo, hi))
                OS[w, h, x, yp] = padded(jnp.where(gy == 0, hi, lo))
            return carry

        lax.fori_loop(0, 4, one, 0)
        out_copy(w, h).start()

    def each(body):
        def one(h, carry):
            body(h)
            return carry

        lax.fori_loop(0, 2, one, 0)

    rise_up, rise_down = (up_x, gy, z_up[2]), (up_x, gy, z_down[2])
    up, down = jnp.zeros((8, L), F32), jnp.zeros((8, L), F32)
    for xi in range(1, 5):
        for yp in range(2):
            j = 2 * xi + yp
            up = jnp.where(zlane8 == j, roll(SN[xi, yp, 1], j - 15), up)
            down = jnp.where(zlane8 == j, roll(SN[xi, yp, 0], j), down)
    su[...] = up
    sd[...] = down
    s_copies = [
        copy(SINIT, su, hsl, z_up), copy(SINIT + 1, sd, hsu, z_down),
        copy(SRISE, su, hslx, rise_up), copy(SRISE + 1, sd, hsux, rise_down),
    ]
    for c in s_copies:
        c.start()

    def rise_copies(h):
        return (
            copy(RISE + 2 * h, PU.at[h], HLX.at[h], rise_up),
            copy(RISE + 2 * h + 1, PD.at[h], HUX.at[h], rise_down),
        )

    def first_edges(h):
        pre(h, 1)
        for c in rise_copies(h):
            c.start()

    each(first_edges)
    for c in shifts:
        c.wait()
    for h in range(2):
        for yp in range(2):
            for zp, tile in enumerate(joined(xr[0, h, yp], xr[1, h, yp])):
                R[h, 3, yp, zp] = tile[:F]
                if h == 0:
                    keep_coef(0, yp, zp, tile)
    for c in s_copies:
        c.wait()
    for xi in range(5):
        for yp in range(2):
            lower, upper, j = (hsl, hsu, 2 * xi + yp) if xi else (hslx, hsux, 8 + yp)
            SEP[xi, yp] = jnp.where(zlane8 == 15, roll(upper[...], 15 - j), roll(SN[xi, yp, 0], -1))
            SOM[xi, yp] = jnp.where(zlane8 == 0, roll(lower[...], -j), roll(SN[xi, yp, 1], 1))

    def entry_edges(h):
        for c in pre_copies(h) + rise_copies(h):
            c.wait()
        low = jnp.zeros((F, L), F32)
        for yp in range(2):
            low = jnp.where(zlane == yp, roll(times(SN, (0, yp, 1), R[h, 3, yp, 1]), yp - 15), low)
        for edge, beyond in ((HL, HLX), (HU, HUX), (PU, None)):
            kept = roll(edge[h].astype(F32)[:F], 2)
            new = low if beyond is None else roll(beyond[h].astype(F32)[:F], -6)
            edge[h] = padded(jnp.where(zlane < 2, new, jnp.where(zlane < 8, kept, 0.0)))

    each(entry_edges)

    def round_of_four(a, carry):
        for b in range(2):

            def even(h):
                if b:
                    for c in pre_copies(h):
                        c.wait()
                solve(h, a, b, 0)

            def odd(h):
                update(h, a, 0)
                solve(h, a, b, 1)

            def between(h):
                update(h, a, 1)
                pre(h, a)

            each(even)
            each(odd)
            if b == 0:
                each(between)

        @pl.when(a == 1)
        def _():
            def add_shifted(h):
                mid_copy(h, 1).wait()
                for yp in range(2):
                    for zp in range(2):
                        S[h, 3, yp, zp] += MR[h, 1, yp, zp][:F].astype(F32)
                leave(0, h, S)

            each(add_shifted)

        def end(h):
            update(h, a, 1)

            @pl.when(a == 0)
            def _():
                for which, field in enumerate((R, S)):
                    for yp in range(2):
                        for zp in range(2):
                            MS[h, which, yp, zp] = padded(field[h, 3, yp, zp])
                    mid_copy(h, which).start()
                    if which == 0:
                        pre(h, 0)
                        for c in slant_copies(h):
                            c.start()
                S[h, 3] = jnp.zeros((2, 2, F, L), F32)

            @pl.when(a == 1)
            def _():
                leave(1, h, R)

        each(end)

        @pl.when(a == 0)
        def _():
            def shifted(h):
                mid_copy(h, 0).wait()
                top = jnp.zeros((F, L), F32)
                for yp in range(2):
                    for zp in range(2):
                        R[h, 3, yp, zp] = MR[h, 0, yp, zp][:F].astype(F32)
                    tile = times(SN, (4, yp, 1), MR[h, 0, yp, 1][:F].astype(F32))
                    top = jnp.where(zlane == 6 + yp, roll(tile, yp - 9), top)
                for c in pre_copies(h) + slant_copies(h):
                    c.wait()
                for edge, upper in ((HL, HLX[h].astype(F32)[:F]), (HU, HUX[h].astype(F32)[:F]), (PU, None)):
                    lower = roll(edge[h].astype(F32)[:F], -2)
                    upper = top if upper is None else roll(upper, 6)
                    edge[h] = padded(jnp.where(zlane < 6, lower, jnp.where(zlane < 8, upper, 0.0)))

            each(shifted)

        return carry

    lax.fori_loop(0, 2, round_of_four, 0)
    stores = [pltpu.make_async_copy(OIN.at[w], out_ref.at[w], out_sem.at[w]) for w in range(2)]
    for w in range(2):
        for h in range(2):
            out_copy(w, h).wait()
        stores[w].start()
    for c in stores:
        c.wait()


def finish(in_any, sol_any, res_any, in_ref, sol_ref, res_ref, perm, in_sem, out_sem):
    loads = [pltpu.make_async_copy(in_any.at[w], in_ref.at[w], in_sem.at[w]) for w in range(2)]
    for c in loads:
        c.start()
    perm[...] = one_hot((512, 512), lambda r, c: source_of(r) == c)
    outs = ((sol_ref, sol_any), (res_ref, res_any))
    stores = [pltpu.make_async_copy(spaced(src), dst, out_sem.at[w]) for w, (src, dst) in enumerate(outs)]
    for w, (out_ref, _) in enumerate(outs):
        loads[w].wait()

        def one(x, carry):
            tiles = jnp.concatenate(
                [jnp.concatenate([in_ref[w, r, x, yp] for r in range(4)], axis=1) for yp in range(2)], axis=0
            )
            back = jnp.dot(tiles, perm[...], preferred_element_type=F32)
            for yp in range(2):
                for y in range(4):
                    out_ref[pl.ds(x * 8 + 2 * y + yp, Q, PITCH), :] = back[yp * B : yp * B + Q, y * L : y * L + L]
            return carry

        lax.fori_loop(0, 4, one, 0)
        stores[w].start()
    for c in stores:
        c.wait()


def on_device(nx, nz, right_side, cell_coef, cell_matrix, face_coupling, patch_inverse):
    flat = right_side.reshape(Q, 32, L)
    tile = lambda *dims, t=BF16: pltpu.VMEM((*dims, B if t == BF16 else F, L), t)
    whole = pl.BlockSpec(memory_space=pl.ANY)
    ordered = pl.pallas_call(
        functools.partial(kernel, nx, nz),
        out_shape=jax.ShapeDtypeStruct((2, 4, 4, 2, B, L), BF16),
        in_specs=[whole] * 5,
        out_specs=whole,
        scratch_shapes=[
            pltpu.VMEM((Q * PITCH, L), F32),
            pltpu.VMEM((32, 32), F32),
            pltpu.VMEM((8 * Q, 8 * Q), BF16),
            pltpu.VMEM((Q, Q), F32),
            pltpu.VMEM((3, Q, Q), F32),
            pltpu.VMEM((512, 512), BF16),
            pltpu.VMEM((B, 512), F32),
            pltpu.VMEM((2, 32, L), F32),
            pltpu.VMEM((6, 8 * Q, L), F32),
            pltpu.VMEM((8 * B, 8 * B), BF16),
            pltpu.VMEM((8 * F, 8 * B), BF16),
            pltpu.VMEM((8 * F, 8 * B), BF16),
            pltpu.VMEM((L, L), F32),
            pltpu.VMEM((F, 7 * B), BF16),
            *[pltpu.VMEM((F, 6 * B), BF16)] * 2,
            *[pltpu.VMEM((F, B), BF16)] * 2,
            tile(4, 4, 2),
            tile(2, 4, 2),
            tile(2, 4, 2, 2, t=F32),
            tile(2, 4, 2, 2, t=F32),
            pltpu.VMEM((5, 2, 2, 8, L), F32),
            pltpu.VMEM((5, 2, 2, 8, L), F32),
            pltpu.VMEM((5, 2, 8, L), F32),
            pltpu.VMEM((5, 2, 8, L), F32),
            *[pltpu.VMEM((8, L), F32)] * 6,
            tile(2, 2, 2),
            pltpu.VMEM((8 * B, 3 * L), BF16),
            pltpu.VMEM((8 * F, 3 * L), F32),
            *[tile(2, 4, 2, 2)] * 4,
            *[tile(2, 2, 2, 2)] * 2,
            *[tile(2)] * 10,
            *[tile(2, 2, 2, 2)] * 2,
            tile(2, 4, 4, 2),
            tile(2, 2, 4, 2),
            pltpu.SemaphoreType.DMA((COPIES,)),
            pltpu.SemaphoreType.DMA((COPIES,)),
            pltpu.SemaphoreType.DMA((5,)),
            pltpu.SemaphoreType.DMA((2,)),
        ],
        compiler_params=pltpu.CompilerParams(
            collective_id=0, has_side_effects=True, vmem_limit_bytes=67043328
        ),
    )(flat, cell_coef.reshape(32, 32), patch_inverse, cell_matrix, face_coupling)
    sol, res = pl.pallas_call(
        finish,
        out_shape=[jax.ShapeDtypeStruct(flat.shape, F32)] * 2,
        in_specs=[whole],
        out_specs=[whole] * 2,
        scratch_shapes=[
            tile(2, 4, 4, 2),
            *[pltpu.VMEM((Q * PITCH, L), F32)] * 2,
            pltpu.VMEM((512, 512), BF16),
            pltpu.SemaphoreType.DMA((2,)),
            pltpu.SemaphoreType.DMA((2,)),
        ],
        compiler_params=pltpu.CompilerParams(vmem_limit_bytes=67043328),
    )(ordered)
    return sol.reshape(right_side.shape), res.reshape(right_side.shape)


def solution(mesh):
    fields = P(None, "gx", "gy", "gz")
    return jax.shard_map(
        functools.partial(on_device, mesh.shape["gx"], mesh.shape["gz"]),
        mesh=mesh,
        in_specs=(fields, P("gx", "gy", "gz"), P(), P(), P()),
        out_specs=(fields, fields),
        check_vma=False,
    )
```

```python
import functools

import jax
import jax.numpy as jnp
from jax import lax
from jax.experimental import pallas as pl
from jax.experimental.pallas import tpu as pltpu
from jax.sharding import PartitionSpec as P

Q = 81
F = 88
B = 96
L = 128
PITCH = 40
F32, BF16 = jnp.float32, jnp.bfloat16
MESH = pl.DeviceIdType.MESH

SWAP, SINIT, SHIFT, PRE, POSTX, POSTZ, MID, OUTS, SLANT, RISE, SRISE, COPIES = 0, 1, 3, 5, 9, 17, 21, 25, 29, 33, 37, 39


def padded(tile):
    return jnp.concatenate([tile, jnp.zeros((B - F, tile.shape[1]), F32)], axis=0).astype(BF16)


def roll(tile, shift):
    shift = shift % L
    return pltpu.roll(tile, shift, 1) if shift else tile


def spaced(ref):
    return ref.reshape(Q, PITCH, L).at[:, :32, :]


def one_hot(shape, hit):
    rows = lax.broadcasted_iota(jnp.int32, shape, 0)
    cols = lax.broadcasted_iota(jnp.int32, shape, 1)
    return jnp.where(hit(rows, cols), 1.0, 0.0).astype(BF16)


def source_of(n):
    return ((n >> 4) & 3) * 128 + (n & 15) * 8 + ((n >> 6) & 1) * 4 + (n >> 7)


def kernel(
    nx, nz,
    b_any, coef_any, p_any, m_any, f_any,
    out_ref,
    b_ref, coef_ref, p_ref, m_ref, f_ref, perm, stage, coefs, p_rows, p_cols, p_stack, PINV, square, W, W_LOW, W_HIGH, W_BELOW, W_ABOVE,
    arrive, partner_in, R, S, SN, CF, SEP, SOM, su, sd, hsl, hsu, hslx, hsux,
    xr, XK, OUT, CB, DB, YR, ZR, XL, XU, PU, PD, HL, HU, QU, QD, GL, GU, HLX, HUX, MS, MR, OIN, OS,
    send_sem, recv_sem, load_sem, out_sem,
):
    gx, gy, gz = lax.axis_index("gx"), lax.axis_index("gy"), lax.axis_index("gz")
    up_x, down_x = lax.rem(gx + 1, nx), lax.rem(gx + nx - 1, nx)
    partner = (gx, 1 - gy, gz)
    x_up, x_down = (up_x, gy, gz), (down_x, gy, gz)
    z_up, z_down = (gx, gy, lax.rem(gz + 1, nz)), (gx, gy, lax.rem(gz + nz - 1, nz))
    cross_up, cross_down = (up_x, 1 - gy, gz), (down_x, 1 - gy, gz)

    def copy(index, src, dst, device):
        return pltpu.make_async_remote_copy(
            src_ref=src, dst_ref=dst, send_sem=send_sem.at[index], recv_sem=recv_sem.at[index],
            device_id=device, device_id_type=MESH,
        )

    loads = [
        pltpu.make_async_copy(src, dst, load_sem.at[i])
        for i, (src, dst) in enumerate(
            ((coef_any, coef_ref), (b_any, spaced(b_ref)), (p_any, p_ref), (m_any, m_ref), (f_any, f_ref))
        )
    ]
    for c in loads:
        c.start()
    slant_up, slant_down = (down_x, gy, z_up[2]), (down_x, gy, z_down[2])
    barrier = pltpu.get_barrier_semaphore()
    for device in (
        partner, x_up, x_down, z_up, z_down, cross_up, cross_down,
        slant_up, slant_down, (up_x, gy, z_up[2]), (up_x, gy, z_down[2]),
    ):
        pl.semaphore_signal(barrier, inc=1, device_id=device, device_id_type=MESH)

    lane = lax.broadcasted_iota(jnp.int32, (F, L), 1)
    zlane = lane & 15
    first, last = zlane == 0, zlane == 15
    half96 = lax.broadcasted_iota(jnp.int32, (B, L), 1) < 64
    zlane8 = lax.broadcasted_iota(jnp.int32, (8, L), 1) & 15

    perm[...] = one_hot((512, 512), lambda r, c: r == source_of(c))
    spread = one_hot((32, L), lambda r, c: r == (c >> 2))
    loads[0].wait()
    coef = coef_ref[...]
    high = coef.astype(BF16)
    low = (coef - high.astype(F32)).astype(BF16)
    coefs[0] = jnp.dot(high, spread, preferred_element_type=F32)
    coefs[1] = jnp.dot(low, spread, preferred_element_type=F32)
    stage[...] = jnp.zeros_like(stage)

    def enter(x):
        for yp in range(2):
            for y in range(4):
                row = x * 8 + 2 * y + yp
                stage[0:Q, y * L : y * L + L] = b_ref[pl.ds(row, Q, PITCH), :]
                stage[Q : Q + 1, y * L : y * L + L] = coefs[0, pl.ds(row, 1), :]
                stage[Q + 1 : Q + 2, y * L : y * L + L] = coefs[1, pl.ds(row, 1), :]
            ordered = jnp.dot(stage[...].astype(BF16), perm[...], preferred_element_type=F32)
            for r in range(4):
                arrive[r, x, yp] = ordered[:, r * L : r * L + L].astype(BF16)

    loads[1].wait()
    enter(3)
    pl.semaphore_wait(barrier, 11)
    shifts = [
        copy(SHIFT, arrive.at[pl.ds(2 * gy, 2), 3], xr.at[0], x_up),
        copy(SHIFT + 1, arrive.at[pl.ds(2 * (1 - gy), 2), 3], xr.at[1], cross_up),
    ]
    for c in shifts:
        c.start()

    def enter_rest(x, carry):
        enter(x)
        return carry

    lax.fori_loop(0, 3, enter_rest, 0)
    swap = copy(SWAP, arrive.at[pl.ds(2 * (1 - gy), 2)], partner_in, partner)
    swap.start()

    for c in loads[2:]:
        c.wait()
    for i in range(6):
        chunk = p_ref[:, i * L : min(i * L + L, 8 * Q)].astype(F32)
        short = L - chunk.shape[1]
        if short:
            chunk = jnp.concatenate([chunk, jnp.zeros((8 * Q, short), F32)], axis=1)
        p_rows[i] = chunk
    for o in range(8):
        for i in range(6):
            rows = p_rows[i, pl.ds(o, Q, 8), :]
            rows = jnp.concatenate([rows, jnp.zeros((F - Q, L), F32)], axis=0)
            p_stack[o * F : o * F + F, i * L : i * L + L] = rows.astype(BF16)
    for i in range(6):
        p_cols[128 * i : 128 * i + 128, :] = one_hot(
            (128, 8 * B), lambda r, c: r + 128 * i == 8 * (c - 96 * ((c * 683) >> 16)) + ((c * 683) >> 16)
        )
    PINV[...] = jnp.dot(p_stack[...], p_cols[...], preferred_element_type=F32).astype(BF16)
    square[...] = jnp.zeros_like(square)
    weights = jnp.zeros((F, 7 * B), F32)
    for i in range(4):
        square[0:Q, 0:Q] = f_ref[i - 1] if i else m_ref[...]
        whole = square[...]
        below, above = (0, 6) if i == 1 else (2 * i - 2, 2 * i - 1)
        parts = [(1, whole)] if i == 0 else [(below, -whole.T), (above, -whole)]
        for at, part in parts:
            place = one_hot((L, 7 * B), lambda r, c: (r + B * at == c) & (r < B))
            weights += jnp.dot(part[:F].astype(BF16), place, preferred_element_type=F32)
    W[...] = weights.astype(BF16)
    W_LOW[...] = weights[:, B:].astype(BF16)
    W_HIGH[...] = weights[:, : 6 * B].astype(BF16)
    W_BELOW[...] = weights[:, :B].astype(BF16)
    W_ABOVE[...] = weights[:, 6 * B :].astype(BF16)
    S[...] = jnp.zeros_like(S)

    def joined(own, other):
        own, other = own.astype(F32), other.astype(F32)
        lo, hi = jnp.where(gy == 0, own, other), jnp.where(gy == 0, other, own)
        return jnp.where(half96, lo, roll(hi, 64)), jnp.where(half96, roll(lo, 64), hi)

    def keep_coef(xi, yp, zp, tile):
        value = jnp.broadcast_to(tile[Q : Q + 1] + tile[Q + 1 : Q + 2], (8, L))
        CF[xi, yp, zp] = value
        SN[xi, yp, zp] = lax.rsqrt(value)

    swap.wait()

    def place(x, carry):
        for h in range(2):
            for yp in range(2):
                for zp, tile in enumerate(joined(arrive[2 * gy + h, x, yp], partner_in[h, x, yp])):
                    R[h, x, yp, zp] = tile[:F]
                    if h == 0:
                        keep_coef(x + 1, yp, zp, tile)
        return carry

    lax.fori_loop(0, 4, place, 0)
    def slot(l, a):
        return (l + 3 * (1 - a)) % 4 if isinstance(a, int) else lax.rem(l + 3 * (1 - a), 4)

    def times(ref, index, tile):
        return ref[index][0:1] * tile

    def pre_copies(h):
        return (
            copy(PRE + 2 * h, PU.at[h], HL.at[h], z_up),
            copy(PRE + 2 * h + 1, PD.at[h], HU.at[h], z_down),
        )

    def x_copy(h, g, a, way):
        if way:
            return copy(POSTX + 4 * h + 2 * g + 1, CB.at[h, slot(0, a)], XU.at[h, g], x_down)
        return copy(POSTX + 4 * h + 2 * g, CB.at[h, slot(3, a)], XL.at[h, g], x_up)

    def z_copies(h):
        return (
            copy(POSTZ + 2 * h, QU.at[h], GL.at[h], z_up),
            copy(POSTZ + 2 * h + 1, QD.at[h], GU.at[h], z_down),
        )

    def mid_copy(h, which):
        return copy(MID + 2 * h + which, MS.at[h, which], MR.at[h, which], x_down)

    def out_copy(w, h):
        return copy(OUTS + 2 * w + h, OS.at[w, h], OIN.at[w, 2 * gy + h], partner)

    def slant_copies(h):
        return (
            copy(SLANT + 2 * h, PU.at[h], HLX.at[h], slant_up),
            copy(SLANT + 2 * h + 1, PD.at[h], HUX.at[h], slant_down),
        )

    def pre(h, a):
        up, down = jnp.zeros((F, L), F32), jnp.zeros((F, L), F32)
        for l in range(4):
            for yp in range(2):
                j = 2 * l + yp
                tile = times(SN, (l + a, yp, 1), R[h, slot(l, a), yp, 1])
                up = jnp.where(zlane == j, roll(tile, j - 15), up)
                tile = times(SN, (l + a, yp, 0), R[h, slot(l, a), yp, 0])
                down = jnp.where(zlane == j, roll(tile, j), down)
        PU[h] = padded(up)
        PD[h] = padded(down)
        for c in pre_copies(h):
            c.start()

    def frames(b, g):
        for dx in range(2):
            for dy in range(2):
                for dz in range(2):
                    yp, zp = (dy if b else 1 - dy), (dz if g else 1 - dz)
                    ry, rz = int(not b and dy == 0), int(not g and dz == 0)
                    yield 4 * dx + 2 * dy + dz, dx, yp, zp, ry, rz

    def solve(h, a, b, g):
        for k, dx, yp, zp, ry, rz in frames(b, g):
            for X in range(2):
                l = 2 * X + dx
                tile = times(SN, (l + a, yp, zp), R[h, slot(l, a), yp, zp])
                tile = roll(tile, 16 * ry + rz)
                if rz:
                    ghost = roll(HL[h].astype(F32)[:F], 16 * ry - (2 * l + yp))
                    tile = jnp.where(first, ghost, tile)
                XK[k * B : k * B + B, X * L : X * L + L] = padded(tile)
            if g == 0:
                edge = (PU if rz else HU)[h].astype(F32)
                XK[k * B : k * B + B, 2 * L : 3 * L] = roll(edge, 16 * ry - (2 * dx + yp)).astype(BF16)
        width = 256 if g else 384
        OUT[:, :width] = jnp.dot(PINV[...], XK[:, :width], preferred_element_type=F32)
        if (b, g) != (0, 0):
            settle(h, a, 1 - g)
        up, down = jnp.zeros((F, L), F32), jnp.zeros((F, L), F32)
        for X, side in ((0, 0), (1, 1), (0, 1), (1, 0)):
            for k, dx, yp, zp, ry, rz in frames(b, g):
                if dx != side:
                    continue
                l = 2 * X + dx
                j = 2 * l + yp
                s = slot(l, a)
                block = OUT[k * F : k * F + F, X * L : X * L + L]
                if g:
                    corr = times(SN, (l + a, yp, zp), roll(block, -16 * ry))
                    if zp:
                        up = jnp.where(zlane == j, roll(corr, j - 15), up)
                        beside = roll(corr, 1)
                    else:
                        down = jnp.where(zlane == j, roll(corr, j), down)
                        beside = roll(corr, -1)
                else:
                    edge = OUT[k * F : k * F + F, 2 * L : 3 * L]
                    here = roll(block, -16 * ry)
                    above = jnp.where(last, roll(edge, 15 - 4 * X - 16 * ry), roll(block, -16 * ry - 1))
                    if zp:
                        corr = times(SN, (l + a, yp, 1), above)
                        beside = times(SOM, (l + a, yp), here)
                    else:
                        corr = times(SN, (l + a, yp, 0), here)
                        beside = times(SEP, (l + a, yp), above)
                S[h, s, yp, zp] += corr
                CB[h, s, yp, zp] = padded(corr)
                DB[h, s, yp, zp] = padded(times(CF, (l + a, yp, zp), corr))
                YR[h, s, yp, zp] = padded(roll(corr, 16 if yp else -16))
                ZR[h, s, yp, zp] = padded(beside)
            if X == side:
                x_copy(h, g, a, 1 - X).start()
        if g:
            QU[h] = padded(up)
            QD[h] = padded(down)
            for c in z_copies(h):
                c.start()

    def pair(ref, *index):
        return jnp.concatenate([ref[(*index, 0)], ref[(*index, 1)]], axis=1)

    def subtract(h, s, yp, weights, blocks):
        stacked = jnp.concatenate(blocks, axis=0) if len(blocks) > 1 else blocks[0]
        change = jnp.dot(weights[...], stacked, preferred_element_type=F32)
        R[h, s, yp, 0] -= change[:, :L]
        R[h, s, yp, 1] -= change[:, L:]

    def update(h, a, g):
        if g:
            for c in z_copies(h):
                c.wait_recv()
        for l in (0, 3, 1, 2):
            s = slot(l, a)
            for yp in range(2):
                j = 2 * l + yp
                even, odd = CB[h, s, yp, 0], CB[h, s, yp, 1]
                behind, ahead = ZR[h, s, yp, 1], ZR[h, s, yp, 0]
                if g:
                    ghost = roll(GL[h].astype(F32)[:F], -j)
                    behind = padded(jnp.where(first, ghost, behind.astype(F32)[:F]))
                    ghost = roll(GU[h].astype(F32)[:F], 15 - j)
                    ahead = padded(jnp.where(last, ghost, ahead.astype(F32)[:F]))
                blocks = [
                    pair(DB, h, s, yp),
                    pair(CB, h, s, 0) if yp else pair(YR, h, s, 1),
                    pair(YR, h, s, 0) if yp else pair(CB, h, s, 1),
                    jnp.concatenate([behind, even], axis=1),
                    jnp.concatenate([odd, ahead], axis=1),
                ]
                if l:
                    blocks = [pair(CB, h, slot(l - 1, a), yp)] + blocks
                if l < 3:
                    blocks = blocks + [pair(CB, h, slot(l + 1, a), yp)]
                subtract(h, s, yp, {0: W_LOW, 3: W_HIGH}.get(l, W), blocks)
        for way, (l, ghost, weights) in enumerate(((3, XL, W_BELOW), (0, XU, W_ABOVE))):
            x_copy(h, g, a, way).wait_recv()
            for yp in range(2):
                subtract(h, slot(3 - l, a), yp, weights, [pair(ghost, h, g, yp)])

    def settle(h, a, g):
        for c in (x_copy(h, g, a, 0), x_copy(h, g, a, 1)) + (z_copies(h) if g else ()):
            c.wait_send()

    def leave(w, h, field):
        def one(x, carry):
            for yp in range(2):
                even, odd = field[h, x, yp, 0], field[h, x, yp, 1]
                lo = jnp.where(lane < 64, even, roll(odd, 64))
                hi = jnp.where(lane < 64, roll(even, 64), odd)
                OIN[w, 2 * gy + h, x, yp] = padded(jnp.where(gy == 0, lo, hi))
                OS[w, h, x, yp] = padded(jnp.where(gy == 0, hi, lo))
            return carry

        lax.fori_loop(0, 4, one, 0)
        out_copy(w, h).start()

    def each(body):
        def one(h, carry):
            body(h)
            return carry

        lax.fori_loop(0, 2, one, 0)

    rise_up, rise_down = (up_x, gy, z_up[2]), (up_x, gy, z_down[2])
    up, down = jnp.zeros((8, L), F32), jnp.zeros((8, L), F32)
    for xi in range(1, 5):
        for yp in range(2):
            j = 2 * xi + yp
            up = jnp.where(zlane8 == j, roll(SN[xi, yp, 1], j - 15), up)
            down = jnp.where(zlane8 == j, roll(SN[xi, yp, 0], j), down)
    su[...] = up
    sd[...] = down
    s_copies = [
        copy(SINIT, su, hsl, z_up), copy(SINIT + 1, sd, hsu, z_down),
        copy(SRISE, su, hslx, rise_up), copy(SRISE + 1, sd, hsux, rise_down),
    ]
    for c in s_copies:
        c.start()

    def rise_copies(h):
        return (
            copy(RISE + 2 * h, PU.at[h], HLX.at[h], rise_up),
            copy(RISE + 2 * h + 1, PD.at[h], HUX.at[h], rise_down),
        )

    def first_edges(h):
        pre(h, 1)
        for c in rise_copies(h):
            c.start()

    each(first_edges)
    for c in shifts:
        c.wait()
    for h in range(2):
        for yp in range(2):
            for zp, tile in enumerate(joined(xr[0, h, yp], xr[1, h, yp])):
                R[h, 3, yp, zp] = tile[:F]
                if h == 0:
                    keep_coef(0, yp, zp, tile)
    for c in s_copies:
        c.wait()
    for xi in range(5):
        for yp in range(2):
            lower, upper, j = (hsl, hsu, 2 * xi + yp) if xi else (hslx, hsux, 8 + yp)
            SEP[xi, yp] = jnp.where(zlane8 == 15, roll(upper[...], 15 - j), roll(SN[xi, yp, 0], -1))
            SOM[xi, yp] = jnp.where(zlane8 == 0, roll(lower[...], -j), roll(SN[xi, yp, 1], 1))

    def entry_edges(h):
        for c in pre_copies(h) + rise_copies(h):
            c.wait()
        low = jnp.zeros((F, L), F32)
        for yp in range(2):
            low = jnp.where(zlane == yp, roll(times(SN, (0, yp, 1), R[h, 3, yp, 1]), yp - 15), low)
        for edge, beyond in ((HL, HLX), (HU, HUX), (PU, None)):
            kept = roll(edge[h].astype(F32)[:F], 2)
            new = low if beyond is None else roll(beyond[h].astype(F32)[:F], -6)
            edge[h] = padded(jnp.where(zlane < 2, new, jnp.where(zlane < 8, kept, 0.0)))

    each(entry_edges)

    def round_of_four(a, carry):
        for b in range(2):

            def even(h):
                if b:
                    for c in pre_copies(h):
                        c.wait()
                solve(h, a, b, 0)

            def odd(h):
                update(h, a, 0)
                solve(h, a, b, 1)

            def between(h):
                update(h, a, 1)
                pre(h, a)

            each(even)
            each(odd)
            if b == 0:
                each(between)

        @pl.when(a == 1)
        def _():
            def add_shifted(h):
                mid_copy(h, 1).wait()
                for yp in range(2):
                    for zp in range(2):
                        S[h, 3, yp, zp] += MR[h, 1, yp, zp][:F].astype(F32)
                leave(0, h, S)

            each(add_shifted)

        def end(h):
            update(h, a, 1)

            @pl.when(a == 0)
            def _():
                for which, field in enumerate((R, S)):
                    for yp in range(2):
                        for zp in range(2):
                            MS[h, which, yp, zp] = padded(field[h, 3, yp, zp])
                    mid_copy(h, which).start()
                    if which == 0:
                        pre(h, 0)
                        for c in slant_copies(h):
                            c.start()
                S[h, 3] = jnp.zeros((2, 2, F, L), F32)

            @pl.when(a == 1)
            def _():
                leave(1, h, R)

            settle(h, a, 1)

        each(end)

        @pl.when(a == 0)
        def _():
            def shifted(h):
                mid_copy(h, 0).wait()
                top = jnp.zeros((F, L), F32)
                for yp in range(2):
                    for zp in range(2):
                        R[h, 3, yp, zp] = MR[h, 0, yp, zp][:F].astype(F32)
                    tile = times(SN, (4, yp, 1), MR[h, 0, yp, 1][:F].astype(F32))
                    top = jnp.where(zlane == 6 + yp, roll(tile, yp - 9), top)
                for c in pre_copies(h) + slant_copies(h):
                    c.wait()
                for edge, upper in ((HL, HLX[h].astype(F32)[:F]), (HU, HUX[h].astype(F32)[:F]), (PU, None)):
                    lower = roll(edge[h].astype(F32)[:F], -2)
                    upper = top if upper is None else roll(upper, 6)
                    edge[h] = padded(jnp.where(zlane < 6, lower, jnp.where(zlane < 8, upper, 0.0)))

            each(shifted)

        return carry

    lax.fori_loop(0, 2, round_of_four, 0)
    stores = [pltpu.make_async_copy(OIN.at[w], out_ref.at[w], out_sem.at[w]) for w in range(2)]
    for w in range(2):
        for h in range(2):
            out_copy(w, h).wait()
        stores[w].start()
    for c in stores:
        c.wait()


def finish(in_any, sol_any, res_any, in_ref, sol_ref, res_ref, perm, in_sem, out_sem):
    loads = [pltpu.make_async_copy(in_any.at[w], in_ref.at[w], in_sem.at[w]) for w in range(2)]
    for c in loads:
        c.start()
    perm[...] = one_hot((512, 512), lambda r, c: source_of(r) == c)
    outs = ((sol_ref, sol_any), (res_ref, res_any))
    stores = [pltpu.make_async_copy(spaced(src), dst, out_sem.at[w]) for w, (src, dst) in enumerate(outs)]
    for w, (out_ref, _) in enumerate(outs):
        loads[w].wait()

        def one(x, carry):
            tiles = jnp.concatenate(
                [jnp.concatenate([in_ref[w, r, x, yp] for r in range(4)], axis=1) for yp in range(2)], axis=0
            )
            back = jnp.dot(tiles, perm[...], preferred_element_type=F32)
            for yp in range(2):
                for y in range(4):
                    out_ref[pl.ds(x * 8 + 2 * y + yp, Q, PITCH), :] = back[yp * B : yp * B + Q, y * L : y * L + L]
            return carry

        lax.fori_loop(0, 4, one, 0)
        stores[w].start()
    for c in stores:
        c.wait()


def on_device(nx, nz, right_side, cell_coef, cell_matrix, face_coupling, patch_inverse):
    flat = right_side.reshape(Q, 32, L)
    tile = lambda *dims, t=BF16: pltpu.VMEM((*dims, B if t == BF16 else F, L), t)
    whole = pl.BlockSpec(memory_space=pl.ANY)
    ordered = pl.pallas_call(
        functools.partial(kernel, nx, nz),
        out_shape=jax.ShapeDtypeStruct((2, 4, 4, 2, B, L), BF16),
        in_specs=[whole] * 5,
        out_specs=whole,
        scratch_shapes=[
            pltpu.VMEM((Q * PITCH, L), F32),
            pltpu.VMEM((32, 32), F32),
            pltpu.VMEM((8 * Q, 8 * Q), BF16),
            pltpu.VMEM((Q, Q), F32),
            pltpu.VMEM((3, Q, Q), F32),
            pltpu.VMEM((512, 512), BF16),
            pltpu.VMEM((B, 512), F32),
            pltpu.VMEM((2, 32, L), F32),
            pltpu.VMEM((6, 8 * Q, L), F32),
            pltpu.VMEM((8 * B, 8 * B), BF16),
            pltpu.VMEM((8 * F, 8 * B), BF16),
            pltpu.VMEM((8 * F, 8 * B), BF16),
            pltpu.VMEM((L, L), F32),
            pltpu.VMEM((F, 7 * B), BF16),
            *[pltpu.VMEM((F, 6 * B), BF16)] * 2,
            *[pltpu.VMEM((F, B), BF16)] * 2,
            tile(4, 4, 2),
            tile(2, 4, 2),
            tile(2, 4, 2, 2, t=F32),
            tile(2, 4, 2, 2, t=F32),
            pltpu.VMEM((5, 2, 2, 8, L), F32),
            pltpu.VMEM((5, 2, 2, 8, L), F32),
            pltpu.VMEM((5, 2, 8, L), F32),
            pltpu.VMEM((5, 2, 8, L), F32),
            *[pltpu.VMEM((8, L), F32)] * 6,
            tile(2, 2, 2),
            pltpu.VMEM((8 * B, 3 * L), BF16),
            pltpu.VMEM((8 * F, 3 * L), F32),
            *[tile(2, 4, 2, 2)] * 4,
            *[tile(2, 2, 2, 2)] * 2,
            *[tile(2)] * 10,
            *[tile(2, 2, 2, 2)] * 2,
            tile(2, 4, 4, 2),
            tile(2, 2, 4, 2),
            pltpu.SemaphoreType.DMA((COPIES,)),
            pltpu.SemaphoreType.DMA((COPIES,)),
            pltpu.SemaphoreType.DMA((5,)),
            pltpu.SemaphoreType.DMA((2,)),
        ],
        compiler_params=pltpu.CompilerParams(
            collective_id=0, has_side_effects=True, vmem_limit_bytes=67043328
        ),
    )(flat, cell_coef.reshape(32, 32), patch_inverse, cell_matrix, face_coupling)
    sol, res = pl.pallas_call(
        finish,
        out_shape=[jax.ShapeDtypeStruct(flat.shape, F32)] * 2,
        in_specs=[whole],
        out_specs=[whole] * 2,
        scratch_shapes=[
            tile(2, 4, 4, 2),
            *[pltpu.VMEM((Q * PITCH, L), F32)] * 2,
            pltpu.VMEM((512, 512), BF16),
            pltpu.SemaphoreType.DMA((2,)),
            pltpu.SemaphoreType.DMA((2,)),
        ],
        compiler_params=pltpu.CompilerParams(vmem_limit_bytes=67043328),
    )(ordered)
    return sol.reshape(right_side.shape), res.reshape(right_side.shape)


def solution(mesh):
    fields = P(None, "gx", "gy", "gz")
    return jax.shard_map(
        functools.partial(on_device, mesh.shape["gx"], mesh.shape["gz"]),
        mesh=mesh,
        in_specs=(fields, P("gx", "gy", "gz"), P(), P(), P()),
        out_specs=(fields, fields),
        check_vma=False,
    )
```
